128 devices in a mesh: dp: 1, tp: 2 (over core), sp: 64 (over z, y, x).
Axes of the slice: x: 4, y: 4, z: 4, core: 2. Of those that a mesh axis runs over, the one named last changes fastest.
Arguments:
- hidden: bfloat16 [64, 2048], P('dp')
- seq_lens: int32 [64], P('dp')
- k_cache: bfloat16 [64, 2, 8192, 128], P('dp', 'tp', 'sp')
- v_cache: bfloat16 [64, 2, 8192, 128], P('dp', 'tp', 'sp')
- attn_norm: bfloat16 [2048], replicated
- w_q: bfloat16 [2048, 2048], P(None, 'tp')
- w_k: bfloat16 [2048, 256], P(None, 'tp')
- w_v: bfloat16 [2048, 256], P(None, 'tp')
- w_o: bfloat16 [2048, 2048], P('tp')
- mlp_norm: bfloat16 [2048], replicated
- w_gate: bfloat16 [2048, 11008], P(None, 'tp')
- w_up: bfloat16 [2048, 11008], P(None, 'tp')
- w_down: bfloat16 [11008, 2048], P('tp')
Outputs:
- output 1: bfloat16 [64, 2048], P('dp')
- output 2: bfloat16 [64, 2, 8192, 128], P('dp', 'tp', 'sp')
- output 3: bfloat16 [64, 2, 8192, 128], P('dp', 'tp', 'sp')
All inputs are finite; a program needn't handle non-finite values.
Results may differ from the reference program's by a relative error of at most 0.00376563.
Values sent between devices are 32-bit elements.
A program may use at most 1 GiB of HBM per device.

```python
import math
import jax
import jax.numpy as jnp
from jax import lax

BATCH = 64
SEQ = 8192
SEQ_BLOCK = 128
D = 2048
HEADS = 16
KV_HEADS = 2
HEAD = 128
FF = 11008

REP = HEADS // KV_HEADS
NORM_EPS = 1e-6


def draw_lens(key_long, key_tail):
    long_lens = jax.random.randint(key_long, (BATCH,), SEQ // 4, SEQ, dtype=jnp.int32)
    tail_lens = SEQ - 1 - jax.random.randint(key_tail, (BATCH,), 0, SEQ_BLOCK, dtype=jnp.int32)
    odd_rows = (jnp.arange(BATCH) % 2) == 1
    seq_lens = jnp.where(odd_rows, tail_lens, long_lens)
    return seq_lens.at[BATCH - 1].set(SEQ // 4).at[0].set(SEQ - 1)


def setup_inputs(seed: int = 0, part: int = 0) -> dict:
    part_key = jax.random.fold_in(jax.random.key(seed), part)
    key_hidden, key_kcache, key_vcache, key_long, key_tail = jax.random.split(part_key, 5)
    weight_keys = jax.random.split(jax.random.key(seed + 1), 9)
    hidden = jax.random.normal(key_hidden, (BATCH, D), jnp.float32)
    k_cache = jax.random.normal(key_kcache, (BATCH, KV_HEADS, SEQ, HEAD), jnp.float32)
    v_cache = jax.random.normal(key_vcache, (BATCH, KV_HEADS, SEQ, HEAD), jnp.float32)
    seq_lens = draw_lens(key_long, key_tail)
    attn_norm = 1.0 + 0.3 * jax.random.normal(weight_keys[0], (D,), jnp.float32)
    w_q = jax.random.normal(weight_keys[1], (D, HEADS * HEAD), jnp.float32) * D ** -0.5
    group_mean = jnp.mean(w_q.reshape(D, KV_HEADS, REP, HEAD), axis=2).reshape(D, KV_HEADS * HEAD)
    align = 0.5 * math.log(SEQ) * REP / math.sqrt(HEAD)
    w_k = align * group_mean + jax.random.normal(weight_keys[2], (D, KV_HEADS * HEAD), jnp.float32) * D ** -0.5
    w_v = jax.random.normal(weight_keys[3], (D, KV_HEADS * HEAD), jnp.float32) * D ** -0.5
    out_scale = 0.3 * math.sqrt(SEQ) / math.sqrt(HEADS * HEAD)
    w_o = jax.random.normal(weight_keys[4], (HEADS * HEAD, D), jnp.float32) * out_scale
    mlp_norm = 1.0 + 0.3 * jax.random.normal(weight_keys[5], (D,), jnp.float32)
    w_gate = jax.random.normal(weight_keys[6], (D, FF), jnp.float32) * D ** -0.5
    w_up = jax.random.normal(weight_keys[7], (D, FF), jnp.float32) * D ** -0.5
    w_down = jax.random.normal(weight_keys[8], (FF, D), jnp.float32) * FF ** -0.5
    return {
        'hidden': hidden.astype(jnp.bfloat16),
        'seq_lens': seq_lens,
        'k_cache': k_cache.astype(jnp.bfloat16),
        'v_cache': v_cache.astype(jnp.bfloat16),
        'attn_norm': attn_norm.astype(jnp.bfloat16),
        'w_q': w_q.astype(jnp.bfloat16),
        'w_k': w_k.astype(jnp.bfloat16),
        'w_v': w_v.astype(jnp.bfloat16),
        'w_o': w_o.astype(jnp.bfloat16),
        'mlp_norm': mlp_norm.astype(jnp.bfloat16),
        'w_gate': w_gate.astype(jnp.bfloat16),
        'w_up': w_up.astype(jnp.bfloat16),
        'w_down': w_down.astype(jnp.bfloat16),
    }


def rms_norm(values, gain):
    wide = values.astype(jnp.float32)
    scaled = wide * lax.rsqrt(jnp.mean(wide * wide, axis=-1, keepdims=True) + NORM_EPS)
    return (scaled * gain.astype(jnp.float32)).astype(jnp.bfloat16)


def reference(hidden, seq_lens, k_cache, v_cache, attn_norm, w_q, w_k, w_v, w_o, mlp_norm, w_gate, w_up, w_down):
    normed = rms_norm(hidden, attn_norm)
    query = jnp.dot(normed, w_q, preferred_element_type=jnp.float32).astype(jnp.bfloat16).reshape(BATCH, KV_HEADS, REP, HEAD)
    k_new = jnp.dot(normed, w_k, preferred_element_type=jnp.float32).astype(jnp.bfloat16).reshape(BATCH, KV_HEADS, 1, HEAD)
    v_new = jnp.dot(normed, w_v, preferred_element_type=jnp.float32).astype(jnp.bfloat16).reshape(BATCH, KV_HEADS, 1, HEAD)
    positions = jnp.arange(SEQ)
    new_slot = (positions[None, :] == seq_lens[:, None])[:, None, :, None]
    k_out = jnp.where(new_slot, k_new, k_cache)
    v_out = jnp.where(new_slot, v_new, v_cache)

    def attend(row):
        q_row, keys, values, length = row
        valid = positions <= length
        scores = jnp.einsum('grd,gsd->grs', q_row.astype(jnp.float32), keys.astype(jnp.float32)) * HEAD ** -0.5
        scores = jnp.where(valid, scores, -jnp.inf)
        weights = jnp.exp(scores - jnp.max(scores, axis=-1, keepdims=True))
        total = jnp.sum(weights, axis=-1, keepdims=True)
        mixed = jnp.einsum('grs,gsd->grd', weights.astype(jnp.bfloat16).astype(jnp.float32), values.astype(jnp.float32))
        return (mixed / total).astype(jnp.bfloat16)

    attended = lax.map(attend, (query, k_out, v_out, seq_lens)).reshape(BATCH, HEADS * HEAD)
    mid_hidden = (hidden.astype(jnp.float32) + jnp.dot(attended, w_o, preferred_element_type=jnp.float32)).astype(jnp.bfloat16)
    normed_mid = rms_norm(mid_hidden, mlp_norm)
    gate_proj = jnp.dot(normed_mid, w_gate, preferred_element_type=jnp.float32)
    up_proj = jnp.dot(normed_mid, w_up, preferred_element_type=jnp.float32)
    activated = (jax.nn.silu(gate_proj) * up_proj).astype(jnp.bfloat16)
    hidden_out = (mid_hidden.astype(jnp.float32) + jnp.dot(activated, w_down, preferred_element_type=jnp.float32)).astype(jnp.bfloat16)
    return (hidden_out, k_out, v_out)
```

```python
import functools

import jax
import jax.numpy as jnp
from jax import lax
from jax.experimental import pallas as pl
from jax.experimental.pallas import tpu as pltpu
from jax.sharding import PartitionSpec as P

NORM_EPS = 1e-6
MESH = pl.DeviceIdType.MESH
F32 = jnp.float32
BF16 = jnp.bfloat16
SEQ_CHUNKS = 4
Q_COLS = 256
FF_COLS = 512
FF_SLOTS = 6
OUT_COLS = 512


def rms_norm(wide, gain):
    scaled = wide * lax.rsqrt(jnp.mean(wide * wide, axis=-1, keepdims=True) + NORM_EPS)
    return (scaled * gain).astype(BF16)


def dot(a, b):
    return jnp.dot(a, b, preferred_element_type=F32)


def attention_kernel(lens_ref, hidden_ref, gain_ref, wq_hbm, wk_hbm, wv_hbm, k_hbm, v_hbm,
                     k_out, v_out, mix_ref, stats_ref,
                     wq, wk, wv, kbuf, vbuf, query, k_new, v_new, scores, probs, w_sem, q_sem, k_sem, v_sem, ko_sem, vo_sem):
    rows, block_len, head_dim = kbuf.shape
    repeat = mix_ref.shape[1]
    per = rows // SEQ_CHUNKS
    q_chunks = wq_hbm.shape[1] // Q_COLS
    scale = head_dim ** -0.5
    base = lax.axis_index('sp') * block_len

    def q_copy(c):
        cols = pl.ds(c * Q_COLS, Q_COLS)
        return pltpu.make_async_copy(wq_hbm.at[:, cols], wq.at[:, cols], q_sem.at[c])

    def cache_copy(hbm, buf, sems, c):
        part = pl.ds(c * per, per)
        return pltpu.make_async_copy(hbm.at[part], buf.at[part], sems.at[c])

    def out_copy(buf, hbm, sems, c):
        part = pl.ds(c * per, per)
        return pltpu.make_async_copy(buf.at[part], hbm.at[part], sems.at[c])

    k_weights = pltpu.make_async_copy(wk_hbm, wk, w_sem.at[0])
    v_weights = pltpu.make_async_copy(wv_hbm, wv, w_sem.at[1])
    k_weights.start()
    v_weights.start()
    for c in range(q_chunks):
        q_copy(c).start()
    for c in range(SEQ_CHUNKS):
        cache_copy(k_hbm, kbuf, k_sem, c).start()
    for c in range(SEQ_CHUNKS):
        cache_copy(v_hbm, vbuf, v_sem, c).start()

    normed = rms_norm(hidden_ref[...].astype(F32), gain_ref[...].astype(F32))
    k_weights.wait()
    k_new[...] = dot(normed, wk[...]).astype(BF16).astype(F32)
    v_weights.wait()
    v_new[...] = dot(normed, wv[...]).astype(BF16).astype(F32)
    for c in range(q_chunks):
        q_copy(c).wait()
        part = dot(normed, wq[:, c * Q_COLS:(c + 1) * Q_COLS]).astype(BF16).astype(F32)
        for h in range(Q_COLS // head_dim):
            query[:, c * (Q_COLS // head_dim) + h, :] = part[:, h * head_dim:(h + 1) * head_dim]

    lanes = lax.broadcasted_iota(jnp.int32, (repeat, block_len), 1)
    tile = lax.broadcasted_iota(jnp.int32, (16, head_dim), 0)

    def insert(buf, new, b, slot):
        start = pl.multiple_of(jnp.clip(slot, 0, block_len - 1) // 16 * 16, 16)
        old = buf[b, pl.ds(start, 16), :]
        fresh = jnp.broadcast_to(new[pl.ds(b, 1), :], (16, head_dim)).astype(BF16)
        buf[b, pl.ds(start, 16), :] = jnp.where(tile == slot - start, fresh, old)

    def score_chunk(c, carry):
        cache_copy(k_hbm, kbuf, k_sem, c).wait()
        for i in range(per):
            b = c * per + i
            insert(kbuf, k_new, b, lens_ref[b] - base)
        out_copy(kbuf, k_out, ko_sem, c).start()
        for i in range(per):
            b = c * per + i
            raw = lax.dot_general(query[b].astype(BF16), kbuf[b], (((1,), (1,)), ((), ())), preferred_element_type=F32)
            scores[b] = jnp.where(lanes <= lens_ref[b] - base, raw * scale, -jnp.inf)
        return carry

    lax.fori_loop(0, SEQ_CHUNKS, score_chunk, 0)

    pairs = lax.broadcasted_iota(jnp.int32, (128, block_len), 1)
    group = 128 // repeat
    half = group // 2

    def soft_chunk(c, carry):
        s = scores[pl.ds(c * group, group)].reshape(128, block_len)
        top = jnp.max(s, axis=-1, keepdims=True)
        p = jnp.where(s > -jnp.inf, jnp.exp(s - top), 0.0)
        total = jnp.sum(p, axis=-1, keepdims=True)
        probs[pl.ds(c * group, group)] = p.reshape(group, repeat, block_len)
        flipped = jnp.where(pairs == 0, top, jnp.where(pairs == 1, total, 0.0)).T
        m_row, l_row = flipped[0:1], flipped[1:2]
        low = lax.broadcasted_iota(jnp.int32, (1, 128), 1) < half * repeat
        stats_ref[2 * c] = jnp.where(low, m_row, pltpu.roll(l_row, half * repeat, 1))
        stats_ref[2 * c + 1] = jnp.where(low, pltpu.roll(m_row, half * repeat, 1), l_row)
        return carry

    lax.fori_loop(0, rows // group, soft_chunk, 0)

    def mix_chunk(c, carry):
        cache_copy(v_hbm, vbuf, v_sem, c).wait()
        for i in range(per):
            b = c * per + i
            insert(vbuf, v_new, b, lens_ref[b] - base)
        out_copy(vbuf, v_out, vo_sem, c).start()
        for i in range(per):
            b = c * per + i
            mix_ref[b] = dot(probs[b].astype(BF16), vbuf[b])
        return carry

    lax.fori_loop(0, SEQ_CHUNKS, mix_chunk, 0)
    for c in range(SEQ_CHUNKS):
        out_copy(kbuf, k_out, ko_sem, c).wait()
        out_copy(vbuf, v_out, vo_sem, c).wait()


def attention(hidden, seq_lens, gain, w_q, w_k, w_v, k_cache, v_cache):
    rows, block_len, head_dim = k_cache.shape
    repeat = w_q.shape[1] // head_dim
    whole = pl.BlockSpec(memory_space=pltpu.VMEM)
    raw = pl.BlockSpec(memory_space=pl.ANY)
    return pl.pallas_call(
        attention_kernel,
        name='attention',
        out_shape=(
            jax.ShapeDtypeStruct(k_cache.shape, BF16),
            jax.ShapeDtypeStruct(v_cache.shape, BF16),
            jax.ShapeDtypeStruct((rows, repeat, head_dim), F32),
            jax.ShapeDtypeStruct((2 * rows * repeat // 128, 1, 128), F32),
        ),
        in_specs=[pl.BlockSpec(memory_space=pltpu.SMEM), whole, whole, raw, raw, raw, raw, raw],
        out_specs=(raw, raw, whole, whole),
        scratch_shapes=[
            pltpu.VMEM(w_q.shape, BF16),
            pltpu.VMEM(w_k.shape, BF16),
            pltpu.VMEM(w_v.shape, BF16),
            pltpu.VMEM(k_cache.shape, BF16),
            pltpu.VMEM(v_cache.shape, BF16),
            pltpu.VMEM((rows, repeat, head_dim), F32),
            pltpu.VMEM((rows, head_dim), F32),
            pltpu.VMEM((rows, head_dim), F32),
            pltpu.VMEM((rows, repeat, block_len), F32),
            pltpu.VMEM((rows, repeat, block_len), F32),
            pltpu.SemaphoreType.DMA((2,)),
            pltpu.SemaphoreType.DMA((w_q.shape[1] // Q_COLS,)),
            pltpu.SemaphoreType.DMA((SEQ_CHUNKS,)),
            pltpu.SemaphoreType.DMA((SEQ_CHUNKS,)),
            pltpu.SemaphoreType.DMA((SEQ_CHUNKS,)),
            pltpu.SemaphoreType.DMA((SEQ_CHUNKS,)),
        ],
        compiler_params=pltpu.CompilerParams(vmem_limit_bytes=24 << 20),
    )(seq_lens, hidden, gain, w_q, w_k, w_v, k_cache, v_cache)


def merge_kernel(hidden_ref, mix_ref, stats_ref, gain_ref, wo_hbm, wg_hbm, wu_hbm, wd_hbm, out_ref,
                 got_mix, got_stats, flipped, own, gathered, wo, wg, wu, wd, sent, other, mid_ref, normed_ref, act, sent2, other2,
                 mix_send, mix_recv, st_send, st_recv, own_send, own_recv, o_send, o_recv, d_send, d_recv,
                 wo_sem, g_sem, u_sem, wd_sem):
    rows, repeat, head_dim = mix_ref.shape
    n = rows
    me = lax.axis_index('sp')
    partner = 1 - lax.axis_index('tp')
    inner = wg_hbm.shape[1]
    full = inner // FF_COLS
    tail = inner - full * FF_COLS
    outs = wo_hbm.shape[1] // OUT_COLS
    per_row = 128 // (2 * repeat)

    barrier = pltpu.get_barrier_semaphore()

    def greet(d, carry):
        pl.semaphore_signal(barrier, inc=1, device_id={'sp': lax.rem(me + d, n)}, device_id_type=MESH)
        return carry

    lax.fori_loop(1, n, greet, 0)
    pl.semaphore_signal(barrier, inc=1, device_id={'tp': partner}, device_id_type=MESH)

    wo_copy = pltpu.make_async_copy(wo_hbm, wo, wo_sem)
    wo_copy.start()

    def ff_copies(i, width=FF_COLS):
        slot = lax.rem(i, FF_SLOTS) if not isinstance(i, int) else i % FF_SLOTS
        start = i * FF_COLS if isinstance(i, int) else pl.multiple_of(i * FF_COLS, FF_COLS)
        cols = pl.ds(start, width)
        return (
            pltpu.make_async_copy(wg_hbm.at[:, cols], wg.at[slot, :, pl.ds(0, width)], g_sem.at[slot]),
            pltpu.make_async_copy(wu_hbm.at[:, cols], wu.at[slot, :, pl.ds(0, width)], u_sem.at[slot]),
        )

    def down_copy(c):
        return pltpu.make_async_copy(wd_hbm.at[:, pl.ds(pl.multiple_of(c * OUT_COLS, OUT_COLS), OUT_COLS)], wd.at[c], wd_sem.at[c])

    for i in range(FF_SLOTS):
        for copy in ff_copies(i):
            copy.start()
    for c in range(outs):
        down_copy(c).start()

    pl.semaphore_wait(barrier, n)

    def send_part(d, carry):
        peer = lax.rem(me + d, n)
        pltpu.make_async_remote_copy(mix_ref.at[peer], got_mix.at[me], mix_send, mix_recv, device_id={'sp': peer}, device_id_type=MESH).start()
        pltpu.make_async_remote_copy(stats_ref.at[peer // per_row], got_stats.at[me], st_send, st_recv, device_id={'sp': peer}, device_id_type=MESH).start()
        return carry

    lax.fori_loop(1, n, send_part, 0)
    got_mix[me] = mix_ref[me]
    got_stats[me] = stats_ref[me // per_row]

    def bulk(ref, send, recv):
        span = ref.at[pl.ds(0, n - 1)]
        return pltpu.make_async_remote_copy(span, span, send, recv, device_id={'tp': partner}, device_id_type=MESH)

    bulk(got_stats, st_send, st_recv).wait_recv()
    flipped[...] = got_stats[:, 0, :].T
    first = pl.multiple_of(lax.rem(me, per_row) * repeat, repeat)
    tops = flipped[pl.ds(first, repeat), :]
    totals = flipped[pl.ds(pl.multiple_of(per_row * repeat + first, repeat), repeat), :]
    factor = jnp.exp(tops - jnp.max(tops, axis=-1, keepdims=True))
    total = jnp.sum(factor * totals, axis=-1, keepdims=True)
    bulk(got_mix, mix_send, mix_recv).wait_recv()
    lanes = 4
    sums = [factor[:, s:s + 1] * got_mix[s] for s in range(lanes)]
    for s in range(lanes, n):
        sums[s % lanes] = sums[s % lanes] + factor[:, s:s + 1] * got_mix[s]
    mixed = (sums[0] + sums[1]) + (sums[2] + sums[3])
    row = (mixed / total).astype(BF16).astype(F32)
    own[...] = row
    gathered[me] = row

    def send_own(d, carry):
        pltpu.make_async_remote_copy(own, gathered.at[me], own_send, own_recv, device_id={'sp': lax.rem(me + d, n)}, device_id_type=MESH).start()
        return carry

    lax.fori_loop(1, n, send_own, 0)
    wo_copy.wait()
    bulk(gathered, own_send, own_recv).wait_recv()
    attended = jnp.concatenate([gathered[:, h, :] for h in range(repeat)], axis=-1).astype(BF16)

    def exchange(mine, theirs, send, recv, c):
        return pltpu.make_async_remote_copy(mine.at[c], theirs.at[c], send.at[c], recv.at[c], device_id={'tp': partner}, device_id_type=MESH)

    for c in range(outs):
        sent[c] = dot(attended, wo[:, c * OUT_COLS:(c + 1) * OUT_COLS])
        exchange(sent, other, o_send, o_recv, c).start()
    square = 0.0
    for c in range(outs):
        exchange(sent, other, o_send, o_recv, c).wait_recv()
        cols = slice(c * OUT_COLS, (c + 1) * OUT_COLS)
        mid = (hidden_ref[:, cols].astype(F32) + (sent[c] + other[c])).astype(BF16)
        mid_ref[:, cols] = mid
    normed_ref[...] = rms_norm(mid_ref[...].astype(F32), gain_ref[...].astype(F32))

    def inner_step(slot, start, width):
        normed = normed_ref[...]
        gate = dot(normed, wg[slot, :, :width])
        up = dot(normed, wu[slot, :, :width])
        act[:, pl.ds(start, width)] = (jax.nn.silu(gate) * up).astype(BF16)

    def ff_step(i, carry):
        for copy in ff_copies(i):
            copy.wait()
        slot = lax.rem(i, FF_SLOTS)
        inner_step(slot, pl.multiple_of(i * FF_COLS, FF_COLS), FF_COLS)

        @pl.when(i + FF_SLOTS < full)
        def _():
            for copy in ff_copies(i + FF_SLOTS):
                copy.start()

        if tail:
            @pl.when(i + FF_SLOTS == full)
            def _():
                for copy in ff_copies(full, tail):
                    copy.start()
        return carry

    lax.fori_loop(0, full, ff_step, 0)
    if tail:
        for copy in ff_copies(full, tail):
            copy.wait()
        inner_step(full % FF_SLOTS, full * FF_COLS, tail)

    def down_step(c, carry):
        down_copy(c).wait()
        sent2[c] = dot(act[...], wd[c])
        exchange(sent2, other2, d_send, d_recv, c).start()
        return carry

    lax.fori_loop(0, outs, down_step, 0)
    for c in range(outs):
        exchange(sent2, other2, d_send, d_recv, c).wait_recv()
        cols = slice(c * OUT_COLS, (c + 1) * OUT_COLS)
        out_ref[:, cols] = (mid_ref[:, cols].astype(F32) + (sent2[c] + other2[c])).astype(BF16)

    bulk(got_mix, mix_send, mix_recv).wait_send()
    bulk(got_stats, st_send, st_recv).wait_send()
    bulk(gathered, own_send, own_recv).wait_send()
    for c in range(outs):
        exchange(sent, other, o_send, o_recv, c).wait_send()
        exchange(sent2, other2, d_send, d_recv, c).wait_send()


def merge(hidden, mix, stats, gain, w_o, w_gate, w_up, w_down):
    rows, repeat, head_dim = mix.shape
    width = w_o.shape[1]
    inner = w_gate.shape[1]
    outs = width // OUT_COLS
    whole = pl.BlockSpec(memory_space=pltpu.VMEM)
    raw = pl.BlockSpec(memory_space=pl.ANY)
    dma = pltpu.SemaphoreType.DMA
    return pl.pallas_call(
        merge_kernel,
        name='merge',
        out_shape=jax.ShapeDtypeStruct(hidden.shape, BF16),
        in_specs=[whole, whole, whole, whole, raw, raw, raw, raw],
        out_specs=whole,
        scratch_shapes=[
            pltpu.VMEM(mix.shape, F32),
            pltpu.VMEM((rows, 1, 128), F32),
            pltpu.VMEM((128, rows), F32),
            pltpu.VMEM((repeat, head_dim), F32),
            pltpu.VMEM(mix.shape, F32),
            pltpu.VMEM(w_o.shape, BF16),
            pltpu.VMEM((FF_SLOTS, width, FF_COLS), BF16),
            pltpu.VMEM((FF_SLOTS, width, FF_COLS), BF16),
            pltpu.VMEM((outs, inner, OUT_COLS), BF16),
            pltpu.VMEM((outs, rows, OUT_COLS), F32),
            pltpu.VMEM((outs, rows, OUT_COLS), F32),
            pltpu.VMEM((rows, width), BF16),
            pltpu.VMEM((rows, width), BF16),
            pltpu.VMEM((rows, inner), BF16),
            pltpu.VMEM((outs, rows, OUT_COLS), F32),
            pltpu.VMEM((outs, rows, OUT_COLS), F32),
            dma, dma, dma, dma, dma, dma,
            dma((outs,)), dma((outs,)), dma((outs,)), dma((outs,)),
            dma, dma((FF_SLOTS,)), dma((FF_SLOTS,)), dma((outs,)),
        ],
        compiler_params=pltpu.CompilerParams(collective_id=0, has_side_effects=True, vmem_limit_bytes=63 << 20),
    )(hidden, mix, stats, gain, w_o, w_gate, w_up, w_down)


def solution(mesh):
    cache_spec = P('dp', 'tp', 'sp', None)
    row_spec = P('dp', None)
    col_spec = P(None, 'tp')
    inner_spec = P('tp', None)
    gain_spec = P(None)

    def local_step(hidden, seq_lens, k_cache, v_cache, attn_norm, w_q, w_k, w_v, w_o, mlp_norm, w_gate, w_up, w_down):
        shape = k_cache.shape
        flat = (shape[0] * shape[1], shape[2], shape[3])
        k_out, v_out, mix, stats = attention(hidden, seq_lens, attn_norm[None, :], w_q, w_k, w_v, k_cache.reshape(flat), v_cache.reshape(flat))
        hidden_out = merge(hidden, mix, stats, mlp_norm[None, :], w_o, w_gate, w_up, w_down)
        return hidden_out, k_out.reshape(shape), v_out.reshape(shape)

    return jax.shard_map(local_step, mesh=mesh, in_specs=(row_spec, P('dp'), cache_spec, cache_spec, gain_spec, col_spec, col_spec, col_spec, inner_spec, gain_spec, col_spec, col_spec, inner_spec), out_specs=(row_spec, cache_spec, cache_spec), check_vma=False)
```

```python
import functools

import jax
import jax.numpy as jnp
from jax import lax
from jax.experimental import pallas as pl
from jax.experimental.pallas import tpu as pltpu
from jax.sharding import PartitionSpec as P

NORM_EPS = 1e-6
MESH = pl.DeviceIdType.MESH
F32 = jnp.float32
BF16 = jnp.bfloat16
SEQ_CHUNKS = 4
Q_COLS = 256
FF_COLS = 512
FF_SLOTS = 6
OUT_COLS = 512


def rms_norm(wide, gain):
    scaled = wide * lax.rsqrt(jnp.mean(wide * wide, axis=-1, keepdims=True) + NORM_EPS)
    return (scaled * gain).astype(BF16)


def dot(a, b):
    return jnp.dot(a, b, preferred_element_type=F32)


def stay(*arrays, space=pltpu.HBM):
    return [pltpu.with_memory_space_constraint(x, space) for x in arrays]


def attention_kernel(lens_hbm, hidden_hbm, gain_hbm, wq_hbm, wk_hbm, wv_hbm, k_hbm, v_hbm,
                     k_out, v_out, mix_ref, stats_ref,
                     lens_ref, hidden_ref, gain_ref, wq, wk, wv, kbuf, vbuf, query, k_new, v_new, scores, probs, small_sem, w_sem, q_sem, k_sem, v_sem, ko_sem, vo_sem):
    rows, block_len, head_dim = kbuf.shape
    repeat = mix_ref.shape[1]
    per = rows // SEQ_CHUNKS
    q_chunks = wq_hbm.shape[1] // Q_COLS
    scale = head_dim ** -0.5
    base = lax.axis_index('sp') * block_len

    def q_copy(c):
        cols = pl.ds(c * Q_COLS, Q_COLS)
        return pltpu.make_async_copy(wq_hbm.at[:, cols], wq.at[:, cols], q_sem.at[c])

    def cache_copy(hbm, buf, sems, c):
        part = pl.ds(c * per, per)
        return pltpu.make_async_copy(hbm.at[part], buf.at[part], sems.at[c])

    def out_copy(buf, hbm, sems, c):
        part = pl.ds(c * per, per)
        return pltpu.make_async_copy(buf.at[part], hbm.at[part], sems.at[c])

    small = [pltpu.make_async_copy(src, dst, small_sem.at[i]) for i, (src, dst) in enumerate(
        ((hidden_hbm, hidden_ref), (gain_hbm, gain_ref), (lens_hbm, lens_ref)))]
    for copy in small:
        copy.start()
    k_weights = pltpu.make_async_copy(wk_hbm, wk, w_sem.at[0])
    v_weights = pltpu.make_async_copy(wv_hbm, wv, w_sem.at[1])
    k_weights.start()
    v_weights.start()
    for c in range(q_chunks):
        q_copy(c).start()
    for c in range(SEQ_CHUNKS):
        cache_copy(k_hbm, kbuf, k_sem, c).start()
    for c in range(SEQ_CHUNKS):
        cache_copy(v_hbm, vbuf, v_sem, c).start()

    for copy in small:
        copy.wait()
    normed = rms_norm(hidden_ref[...].astype(F32), gain_ref[...].astype(F32)[None, :])
    k_weights.wait()
    k_new[...] = dot(normed, wk[...]).astype(BF16).astype(F32)
    v_weights.wait()
    v_new[...] = dot(normed, wv[...]).astype(BF16).astype(F32)
    for c in range(q_chunks):
        q_copy(c).wait()
        part = dot(normed, wq[:, c * Q_COLS:(c + 1) * Q_COLS]).astype(BF16).astype(F32)
        for h in range(Q_COLS // head_dim):
            query[:, c * (Q_COLS // head_dim) + h, :] = part[:, h * head_dim:(h + 1) * head_dim]

    lanes = lax.broadcasted_iota(jnp.int32, (repeat, block_len), 1)
    tile = lax.broadcasted_iota(jnp.int32, (16, head_dim), 0)

    def insert(buf, new, b, slot):
        start = pl.multiple_of(jnp.clip(slot, 0, block_len - 1) // 16 * 16, 16)
        old = buf[b, pl.ds(start, 16), :]
        fresh = jnp.broadcast_to(new[pl.ds(b, 1), :], (16, head_dim)).astype(BF16)
        buf[b, pl.ds(start, 16), :] = jnp.where(tile == slot - start, fresh, old)

    def score_chunk(c, carry):
        cache_copy(k_hbm, kbuf, k_sem, c).wait()
        for i in range(per):
            b = c * per + i
            insert(kbuf, k_new, b, lens_ref[b] - base)
        out_copy(kbuf, k_out, ko_sem, c).start()
        for i in range(per):
            b = c * per + i
            raw = lax.dot_general(query[b].astype(BF16), kbuf[b], (((1,), (1,)), ((), ())), preferred_element_type=F32)
            scores[b] = jnp.where(lanes <= lens_ref[b] - base, raw * scale, -jnp.inf)
        return carry

    lax.fori_loop(0, SEQ_CHUNKS, score_chunk, 0)

    pairs = lax.broadcasted_iota(jnp.int32, (128, block_len), 1)
    group = 128 // repeat
    half = group // 2

    def soft_chunk(c, carry):
        s = scores[pl.ds(c * group, group)].reshape(128, block_len)
        top = jnp.max(s, axis=-1, keepdims=True)
        p = jnp.where(s > -jnp.inf, jnp.exp(s - top), 0.0)
        total = jnp.sum(p, axis=-1, keepdims=True)
        probs[pl.ds(c * group, group)] = p.reshape(group, repeat, block_len)
        flipped = jnp.where(pairs == 0, top, jnp.where(pairs == 1, total, 0.0)).T
        m_row, l_row = flipped[0:1], flipped[1:2]
        low = lax.broadcasted_iota(jnp.int32, (1, 128), 1) < half * repeat
        stats_ref[2 * c] = jnp.where(low, m_row, pltpu.roll(l_row, half * repeat, 1))
        stats_ref[2 * c + 1] = jnp.where(low, pltpu.roll(m_row, half * repeat, 1), l_row)
        return carry

    lax.fori_loop(0, rows // group, soft_chunk, 0)

    def mix_chunk(c, carry):
        cache_copy(v_hbm, vbuf, v_sem, c).wait()
        for i in range(per):
            b = c * per + i
            insert(vbuf, v_new, b, lens_ref[b] - base)
        out_copy(vbuf, v_out, vo_sem, c).start()
        for i in range(per):
            b = c * per + i
            mix_ref[b] = dot(probs[b].astype(BF16), vbuf[b])
        return carry

    lax.fori_loop(0, SEQ_CHUNKS, mix_chunk, 0)
    for c in range(SEQ_CHUNKS):
        out_copy(kbuf, k_out, ko_sem, c).wait()
        out_copy(vbuf, v_out, vo_sem, c).wait()


def attention(hidden, seq_lens, gain, w_q, w_k, w_v, k_cache, v_cache):
    rows, block_len, head_dim = k_cache.shape
    repeat = w_q.shape[1] // head_dim
    whole = pl.BlockSpec(memory_space=pltpu.VMEM)
    raw = pl.BlockSpec(memory_space=pltpu.HBM)
    return pl.pallas_call(
        attention_kernel,
        name='attention',
        out_shape=(
            jax.ShapeDtypeStruct(k_cache.shape, BF16),
            jax.ShapeDtypeStruct(v_cache.shape, BF16),
            jax.ShapeDtypeStruct((rows, repeat, head_dim), F32),
            jax.ShapeDtypeStruct((2 * rows * repeat // 128, 1, 128), F32),
        ),
        in_specs=[raw] * 8,
        out_specs=(raw, raw, whole, whole),
        scratch_shapes=[
            pltpu.SMEM(seq_lens.shape, jnp.int32),
            pltpu.VMEM(hidden.shape, BF16),
            pltpu.VMEM(gain.shape, BF16),
            pltpu.VMEM(w_q.shape, BF16),
            pltpu.VMEM(w_k.shape, BF16),
            pltpu.VMEM(w_v.shape, BF16),
            pltpu.VMEM(k_cache.shape, BF16),
            pltpu.VMEM(v_cache.shape, BF16),
            pltpu.VMEM((rows, repeat, head_dim), F32),
            pltpu.VMEM((rows, head_dim), F32),
            pltpu.VMEM((rows, head_dim), F32),
            pltpu.VMEM((rows, repeat, block_len), F32),
            pltpu.VMEM((rows, repeat, block_len), F32),
            pltpu.SemaphoreType.DMA((3,)),
            pltpu.SemaphoreType.DMA((2,)),
            pltpu.SemaphoreType.DMA((w_q.shape[1] // Q_COLS,)),
            pltpu.SemaphoreType.DMA((SEQ_CHUNKS,)),
            pltpu.SemaphoreType.DMA((SEQ_CHUNKS,)),
            pltpu.SemaphoreType.DMA((SEQ_CHUNKS,)),
            pltpu.SemaphoreType.DMA((SEQ_CHUNKS,)),
        ],
        compiler_params=pltpu.CompilerParams(vmem_limit_bytes=30 << 20),
    )(*stay(seq_lens, hidden, gain, w_q, w_k, w_v, k_cache, v_cache))


def merge_kernel(hidden_hbm, mix_ref, stats_ref, gain_hbm, wo_hbm, wg_hbm, wu_hbm, wd_hbm, out_ref,
                 hidden_ref, gain_ref, got_mix, got_stats, flipped, own, gathered, wo, wg, wu, wd, sent, other, mid_ref, normed_ref, act, sent2, other2,
                 mix_send, mix_recv, st_send, st_recv, own_send, own_recv, o_send, o_recv, d_send, d_recv,
                 small_sem, wo_sem, g_sem, u_sem, wd_sem):
    rows, repeat, head_dim = mix_ref.shape
    n = rows
    me = lax.axis_index('sp')
    partner = 1 - lax.axis_index('tp')
    inner = wg_hbm.shape[1]
    full = inner // FF_COLS
    tail = inner - full * FF_COLS
    outs = wo_hbm.shape[1] // OUT_COLS
    per_row = 128 // (2 * repeat)

    barrier = pltpu.get_barrier_semaphore()

    def greet(d, carry):
        pl.semaphore_signal(barrier, inc=1, device_id={'sp': lax.rem(me + d, n)}, device_id_type=MESH)
        return carry

    lax.fori_loop(1, n, greet, 0)
    pl.semaphore_signal(barrier, inc=1, device_id={'tp': partner}, device_id_type=MESH)

    small = [pltpu.make_async_copy(src, dst, small_sem.at[i]) for i, (src, dst) in enumerate(
        ((hidden_hbm, hidden_ref), (gain_hbm, gain_ref)))]
    for copy in small:
        copy.start()
    wo_copy = pltpu.make_async_copy(wo_hbm, wo, wo_sem)
    wo_copy.start()

    def ff_copies(i, width=FF_COLS):
        slot = lax.rem(i, FF_SLOTS) if not isinstance(i, int) else i % FF_SLOTS
        start = i * FF_COLS if isinstance(i, int) else pl.multiple_of(i * FF_COLS, FF_COLS)
        cols = pl.ds(start, width)
        return (
            pltpu.make_async_copy(wg_hbm.at[:, cols], wg.at[slot, :, pl.ds(0, width)], g_sem.at[slot]),
            pltpu.make_async_copy(wu_hbm.at[:, cols], wu.at[slot, :, pl.ds(0, width)], u_sem.at[slot]),
        )

    def down_copy(c):
        return pltpu.make_async_copy(wd_hbm.at[:, pl.ds(pl.multiple_of(c * OUT_COLS, OUT_COLS), OUT_COLS)], wd.at[c], wd_sem.at[c])

    for i in range(FF_SLOTS):
        for copy in ff_copies(i):
            copy.start()
    for c in range(outs):
        down_copy(c).start()

    pl.semaphore_wait(barrier, n)

    def send_part(d, carry):
        peer = lax.rem(me + d, n)
        pltpu.make_async_remote_copy(mix_ref.at[peer], got_mix.at[me], mix_send, mix_recv, device_id={'sp': peer}, device_id_type=MESH).start()
        pltpu.make_async_remote_copy(stats_ref.at[peer // per_row], got_stats.at[me], st_send, st_recv, device_id={'sp': peer}, device_id_type=MESH).start()
        return carry

    lax.fori_loop(1, n, send_part, 0)
    got_mix[me] = mix_ref[me]
    got_stats[me] = stats_ref[me // per_row]

    def bulk(ref, send, recv):
        span = ref.at[pl.ds(0, n - 1)]
        return pltpu.make_async_remote_copy(span, span, send, recv, device_id={'tp': partner}, device_id_type=MESH)

    bulk(got_stats, st_send, st_recv).wait_recv()
    flipped[...] = got_stats[:, 0, :].T
    first = pl.multiple_of(lax.rem(me, per_row) * repeat, repeat)
    tops = flipped[pl.ds(first, repeat), :]
    totals = flipped[pl.ds(pl.multiple_of(per_row * repeat + first, repeat), repeat), :]
    factor = jnp.exp(tops - jnp.max(tops, axis=-1, keepdims=True))
    total = jnp.sum(factor * totals, axis=-1, keepdims=True)
    bulk(got_mix, mix_send, mix_recv).wait_recv()
    lanes = 4
    sums = [factor[:, s:s + 1] * got_mix[s] for s in range(lanes)]
    for s in range(lanes, n):
        sums[s % lanes] = sums[s % lanes] + factor[:, s:s + 1] * got_mix[s]
    mixed = (sums[0] + sums[1]) + (sums[2] + sums[3])
    row = (mixed / total).astype(BF16).astype(F32)
    own[...] = row
    gathered[me] = row

    def send_own(d, carry):
        pltpu.make_async_remote_copy(own, gathered.at[me], own_send, own_recv, device_id={'sp': lax.rem(me + d, n)}, device_id_type=MESH).start()
        return carry

    lax.fori_loop(1, n, send_own, 0)
    wo_copy.wait()
    bulk(gathered, own_send, own_recv).wait_recv()
    attended = jnp.concatenate([gathered[:, h, :] for h in range(repeat)], axis=-1).astype(BF16)

    def exchange(mine, theirs, send, recv, c):
        return pltpu.make_async_remote_copy(mine.at[c], theirs.at[c], send.at[c], recv.at[c], device_id={'tp': partner}, device_id_type=MESH)

    for c in range(outs):
        sent[c] = dot(attended, wo[:, c * OUT_COLS:(c + 1) * OUT_COLS])
        exchange(sent, other, o_send, o_recv, c).start()
    for copy in small:
        copy.wait()
    for c in range(outs):
        exchange(sent, other, o_send, o_recv, c).wait_recv()
        cols = slice(c * OUT_COLS, (c + 1) * OUT_COLS)
        mid = (hidden_ref[:, cols].astype(F32) + (sent[c] + other[c])).astype(BF16)
        mid_ref[:, cols] = mid
    normed_ref[...] = rms_norm(mid_ref[...].astype(F32), gain_ref[...].astype(F32)[None, :])

    def inner_step(slot, start, width):
        normed = normed_ref[...]
        gate = dot(normed, wg[slot, :, :width])
        up = dot(normed, wu[slot, :, :width])
        act[:, pl.ds(start, width)] = (jax.nn.silu(gate) * up).astype(BF16)

    def ff_step(i, carry):
        for copy in ff_copies(i):
            copy.wait()
        slot = lax.rem(i, FF_SLOTS)
        inner_step(slot, pl.multiple_of(i * FF_COLS, FF_COLS), FF_COLS)

        @pl.when(i + FF_SLOTS < full)
        def _():
            for copy in ff_copies(i + FF_SLOTS):
                copy.start()

        if tail:
            @pl.when(i + FF_SLOTS == full)
            def _():
                for copy in ff_copies(full, tail):
                    copy.start()
        return carry

    lax.fori_loop(0, full, ff_step, 0)
    if tail:
        for copy in ff_copies(full, tail):
            copy.wait()
        inner_step(full % FF_SLOTS, full * FF_COLS, tail)

    def down_step(c, carry):
        down_copy(c).wait()
        sent2[c] = dot(act[...], wd[c])
        exchange(sent2, other2, d_send, d_recv, c).start()
        return carry

    lax.fori_loop(0, outs, down_step, 0)
    for c in range(outs):
        exchange(sent2, other2, d_send, d_recv, c).wait_recv()
        cols = slice(c * OUT_COLS, (c + 1) * OUT_COLS)
        out_ref[:, cols] = (mid_ref[:, cols].astype(F32) + (sent2[c] + other2[c])).astype(BF16)

    bulk(got_mix, mix_send, mix_recv).wait_send()
    bulk(got_stats, st_send, st_recv).wait_send()
    bulk(gathered, own_send, own_recv).wait_send()
    for c in range(outs):
        exchange(sent, other, o_send, o_recv, c).wait_send()
        exchange(sent2, other2, d_send, d_recv, c).wait_send()


def merge(hidden, mix, stats, gain, w_o, w_gate, w_up, w_down):
    rows, repeat, head_dim = mix.shape
    width = w_o.shape[1]
    inner = w_gate.shape[1]
    outs = width // OUT_COLS
    whole = pl.BlockSpec(memory_space=pltpu.VMEM)
    raw = pl.BlockSpec(memory_space=pltpu.HBM)
    dma = pltpu.SemaphoreType.DMA
    return pl.pallas_call(
        merge_kernel,
        name='merge',
        out_shape=pltpu.VMEM(hidden.shape, BF16),
        in_specs=[raw, whole, whole, raw, raw, raw, raw, raw],
        out_specs=whole,
        scratch_shapes=[
            pltpu.VMEM(hidden.shape, BF16),
            pltpu.VMEM(gain.shape, BF16),
            pltpu.VMEM(mix.shape, F32),
            pltpu.VMEM((rows, 1, 128), F32),
            pltpu.VMEM((128, rows), F32),
            pltpu.VMEM((repeat, head_dim), F32),
            pltpu.VMEM(mix.shape, F32),
            pltpu.VMEM(w_o.shape, BF16),
            pltpu.VMEM((FF_SLOTS, width, FF_COLS), BF16),
            pltpu.VMEM((FF_SLOTS, width, FF_COLS), BF16),
            pltpu.VMEM((outs, inner, OUT_COLS), BF16),
            pltpu.VMEM((outs, rows, OUT_COLS), F32),
            pltpu.VMEM((outs, rows, OUT_COLS), F32),
            pltpu.VMEM((rows, width), BF16),
            pltpu.VMEM((rows, width), BF16),
            pltpu.VMEM((rows, inner), BF16),
            pltpu.VMEM((outs, rows, OUT_COLS), F32),
            pltpu.VMEM((outs, rows, OUT_COLS), F32),
            dma, dma, dma, dma, dma, dma,
            dma((outs,)), dma((outs,)), dma((outs,)), dma((outs,)),
            dma((2,)), dma, dma((FF_SLOTS,)), dma((FF_SLOTS,)), dma((outs,)),
        ],
        compiler_params=pltpu.CompilerParams(collective_id=0, has_side_effects=True, vmem_limit_bytes=58 << 20),
    )(*stay(hidden), *stay(mix, stats, space=pltpu.VMEM), *stay(gain, w_o, w_gate, w_up, w_down))


def solution(mesh):
    cache_spec = P('dp', 'tp', 'sp', None)
    row_spec = P('dp', None)
    col_spec = P(None, 'tp')
    inner_spec = P('tp', None)
    gain_spec = P(None)

    def local_step(hidden, seq_lens, k_cache, v_cache, attn_norm, w_q, w_k, w_v, w_o, mlp_norm, w_gate, w_up, w_down):
        shape = k_cache.shape
        flat = (shape[0] * shape[1], shape[2], shape[3])
        k_out, v_out, mix, stats = attention(hidden, seq_lens, attn_norm, w_q, w_k, w_v, k_cache.reshape(flat), v_cache.reshape(flat))
        hidden_out = merge(hidden, mix, stats, mlp_norm, w_o, w_gate, w_up, w_down)
        return hidden_out, k_out.reshape(shape), v_out.reshape(shape)

    return jax.shard_map(local_step, mesh=mesh, in_specs=(row_spec, P('dp'), cache_spec, cache_spec, gain_spec, col_spec, col_spec, col_spec, inner_spec, gain_spec, col_spec, col_spec, inner_spec), out_specs=(row_spec, cache_spec, cache_spec), check_vma=False)
```

```python
import itertools

import jax
import jax.numpy as jnp
from jax import lax
from jax.experimental import pallas as pl
from jax.experimental.pallas import tpu as pltpu
from jax.sharding import PartitionSpec as P

NORM_EPS = 1e-6
MESH = pl.DeviceIdType.MESH
F32 = jnp.float32
BF16 = jnp.bfloat16
SEQ_CHUNKS = 4
PAD_ROWS = 128
Q_COLS = 256
FF_COLS = 512
FF_SLOTS = 6
OUT_COLS = 512


def rms_norm(wide, gain):
    scaled = wide * lax.rsqrt(jnp.mean(wide * wide, axis=-1, keepdims=True) + NORM_EPS)
    return (scaled * gain).astype(BF16)


def dot(a, b):
    return jnp.dot(a, b, preferred_element_type=F32)


def stay(*arrays, space=pltpu.HBM):
    return [pltpu.with_memory_space_constraint(x, space) for x in arrays]


def attention_kernel(lens_hbm, hidden_hbm, gain_hbm, wq_hbm, wk_hbm, wv_hbm, k_hbm, v_hbm,
                     k_out, v_out, mix_ref, stats_ref,
                     lens_ref, hidden_ref, gain_ref, wq, wk, wv, kbuf, vbuf, query, k_new, v_new, scores, probs, small_sem, w_sem, q_sem, k_sem, v_sem, ko_sem, vo_sem):
    rows, block_len, head_dim = kbuf.shape
    repeat = mix_ref.shape[1]
    per = rows // SEQ_CHUNKS
    q_chunks = wq_hbm.shape[1] // Q_COLS
    scale = head_dim ** -0.5
    base = lax.axis_index('sp') * block_len

    def q_copy(c):
        cols = pl.ds(c * Q_COLS, Q_COLS)
        return pltpu.make_async_copy(wq_hbm.at[:, cols], wq.at[:, cols], q_sem.at[c])

    def cache_copy(hbm, buf, sems, c):
        part = pl.ds(c * per, per)
        return pltpu.make_async_copy(hbm.at[part], buf.at[part], sems.at[c])

    def out_copy(buf, hbm, sems, c):
        part = pl.ds(c * per, per)
        return pltpu.make_async_copy(buf.at[part], hbm.at[part], sems.at[c])

    small = [pltpu.make_async_copy(src, dst, small_sem.at[i]) for i, (src, dst) in enumerate(
        ((hidden_hbm, hidden_ref), (gain_hbm, gain_ref), (lens_hbm, lens_ref)))]
    for copy in small:
        copy.start()
    k_weights = pltpu.make_async_copy(wk_hbm, wk, w_sem.at[0])
    v_weights = pltpu.make_async_copy(wv_hbm, wv, w_sem.at[1])
    k_weights.start()
    v_weights.start()
    for c in range(q_chunks):
        q_copy(c).start()
    for c in range(SEQ_CHUNKS):
        cache_copy(k_hbm, kbuf, k_sem, c).start()
    for c in range(SEQ_CHUNKS):
        cache_copy(v_hbm, vbuf, v_sem, c).start()

    for copy in small:
        copy.wait()
    normed = rms_norm(hidden_ref[...].astype(F32), gain_ref[...].astype(F32)[None, :])
    k_weights.wait()
    k_new[...] = dot(normed, wk[...]).astype(BF16).astype(F32)
    v_weights.wait()
    v_new[...] = dot(normed, wv[...]).astype(BF16).astype(F32)
    for c in range(q_chunks):
        q_copy(c).wait()
        part = dot(normed, wq[:, c * Q_COLS:(c + 1) * Q_COLS]).astype(BF16).astype(F32)
        for h in range(Q_COLS // head_dim):
            query[:, c * (Q_COLS // head_dim) + h, :] = part[:, h * head_dim:(h + 1) * head_dim]

    lanes = lax.broadcasted_iota(jnp.int32, (repeat, block_len), 1)
    tile = lax.broadcasted_iota(jnp.int32, (16, head_dim), 0)

    def insert(buf, new, b, slot):
        start = pl.multiple_of(jnp.clip(slot, 0, block_len - 1) // 16 * 16, 16)
        old = buf[b, pl.ds(start, 16), :]
        fresh = jnp.broadcast_to(new[pl.ds(b, 1), :], (16, head_dim)).astype(BF16)
        buf[b, pl.ds(start, 16), :] = jnp.where(tile == slot - start, fresh, old)

    def score_chunk(c, carry):
        cache_copy(k_hbm, kbuf, k_sem, c).wait()
        for i in range(per):
            b = c * per + i
            insert(kbuf, k_new, b, lens_ref[b] - base)
        out_copy(kbuf, k_out, ko_sem, c).start()
        for i in range(per):
            b = c * per + i
            raw = lax.dot_general(query[b].astype(BF16), kbuf[b], (((1,), (1,)), ((), ())), preferred_element_type=F32)
            scores[b] = jnp.where(lanes <= lens_ref[b] - base, raw * scale, -jnp.inf)
        return carry

    for c in range(SEQ_CHUNKS):
        score_chunk(c, 0)

    pairs = lax.broadcasted_iota(jnp.int32, (128, block_len), 1)
    group = 128 // repeat
    half = group // 2

    def soft_chunk(c, carry):
        s = scores[pl.ds(c * group, group)].reshape(128, block_len)
        top = jnp.max(s, axis=-1, keepdims=True)
        p = jnp.where(s > -jnp.inf, jnp.exp(s - top), 0.0)
        total = jnp.sum(p, axis=-1, keepdims=True)
        probs[pl.ds(c * group, group)] = p.reshape(group, repeat, block_len)
        flipped = jnp.where(pairs == 0, top, jnp.where(pairs == 1, total, 0.0)).T
        m_row, l_row = flipped[0:1], flipped[1:2]
        low = lax.broadcasted_iota(jnp.int32, (1, 128), 1) < half * repeat
        stats_ref[2 * c] = jnp.where(low, m_row, pltpu.roll(l_row, half * repeat, 1))
        stats_ref[2 * c + 1] = jnp.where(low, pltpu.roll(m_row, half * repeat, 1), l_row)
        return carry

    for c in range(rows // group):
        soft_chunk(c, 0)

    def mix_chunk(c, carry):
        cache_copy(v_hbm, vbuf, v_sem, c).wait()
        for i in range(per):
            b = c * per + i
            insert(vbuf, v_new, b, lens_ref[b] - base)
        out_copy(vbuf, v_out, vo_sem, c).start()
        for i in range(per):
            b = c * per + i
            mix_ref[b] = dot(probs[b].astype(BF16), vbuf[b])
        return carry

    for c in range(SEQ_CHUNKS):
        mix_chunk(c, 0)
    for c in range(SEQ_CHUNKS):
        out_copy(kbuf, k_out, ko_sem, c).wait()
        out_copy(vbuf, v_out, vo_sem, c).wait()


def attention(hidden, seq_lens, gain, w_q, w_k, w_v, k_cache, v_cache):
    rows, block_len, head_dim = k_cache.shape
    repeat = w_q.shape[1] // head_dim
    whole = pl.BlockSpec(memory_space=pltpu.VMEM)
    raw = pl.BlockSpec(memory_space=pltpu.HBM)
    return pl.pallas_call(
        attention_kernel,
        name='attention',
        out_shape=(
            jax.ShapeDtypeStruct(k_cache.shape, BF16),
            jax.ShapeDtypeStruct(v_cache.shape, BF16),
            jax.ShapeDtypeStruct((rows, repeat, head_dim), F32),
            jax.ShapeDtypeStruct((2 * rows * repeat // 128, 1, 128), F32),
        ),
        in_specs=[raw] * 8,
        out_specs=(raw, raw, whole, whole),
        scratch_shapes=[
            pltpu.SMEM(seq_lens.shape, jnp.int32),
            pltpu.VMEM(hidden.shape, BF16),
            pltpu.VMEM(gain.shape, BF16),
            pltpu.VMEM(w_q.shape, BF16),
            pltpu.VMEM(w_k.shape, BF16),
            pltpu.VMEM(w_v.shape, BF16),
            pltpu.VMEM(k_cache.shape, BF16),
            pltpu.VMEM(v_cache.shape, BF16),
            pltpu.VMEM((rows, repeat, head_dim), F32),
            pltpu.VMEM((rows, head_dim), F32),
            pltpu.VMEM((rows, head_dim), F32),
            pltpu.VMEM((rows, repeat, block_len), F32),
            pltpu.VMEM((rows, repeat, block_len), F32),
            pltpu.SemaphoreType.DMA((3,)),
            pltpu.SemaphoreType.DMA((2,)),
            pltpu.SemaphoreType.DMA((w_q.shape[1] // Q_COLS,)),
            pltpu.SemaphoreType.DMA((SEQ_CHUNKS,)),
            pltpu.SemaphoreType.DMA((SEQ_CHUNKS,)),
            pltpu.SemaphoreType.DMA((SEQ_CHUNKS,)),
            pltpu.SemaphoreType.DMA((SEQ_CHUNKS,)),
        ],
        compiler_params=pltpu.CompilerParams(vmem_limit_bytes=30 << 20),
    )(*stay(seq_lens, hidden, gain, w_q, w_k, w_v, k_cache, v_cache))


def merge_kernel(hidden_hbm, mix_ref, stats_ref, gain_hbm, wo_hbm, wg_hbm, wu_hbm, wd_hbm, out_ref,
                 hidden_ref, gain_ref, got_mix, got_stats, flipped, own, gathered, wo, wg, wu, wd, sent, other, mid_ref, normed_ref, act, sent2, other2,
                 mix_send, mix_recv, st_send, st_recv, own_send, own_recv, o_send, o_recv, d_send, d_recv,
                 small_sem, wo_sem, g_sem, u_sem, wd_sem):
    rows, repeat, head_dim = mix_ref.shape
    n = rows
    me = lax.axis_index('sp')
    partner = 1 - lax.axis_index('tp')
    inner = wg_hbm.shape[1]
    full = inner // FF_COLS
    tail = inner - full * FF_COLS
    outs = wo_hbm.shape[1] // OUT_COLS
    per_row = 128 // (2 * repeat)

    barrier = pltpu.get_barrier_semaphore()

    def greet(d, carry):
        pl.semaphore_signal(barrier, inc=1, device_id={'sp': lax.rem(me + d, n)}, device_id_type=MESH)
        return carry

    lax.fori_loop(1, n, greet, 0)
    pl.semaphore_signal(barrier, inc=1, device_id={'tp': partner}, device_id_type=MESH)

    small = [pltpu.make_async_copy(src, dst, small_sem.at[i]) for i, (src, dst) in enumerate(
        ((hidden_hbm, hidden_ref), (gain_hbm, gain_ref)))]
    for copy in small:
        copy.start()
    wo_copy = pltpu.make_async_copy(wo_hbm, wo, wo_sem)
    wo_copy.start()

    def ff_copies(i, width=FF_COLS):
        slot = lax.rem(i, FF_SLOTS) if not isinstance(i, int) else i % FF_SLOTS
        start = i * FF_COLS if isinstance(i, int) else pl.multiple_of(i * FF_COLS, FF_COLS)
        cols = pl.ds(start, width)
        return (
            pltpu.make_async_copy(wg_hbm.at[:, cols], wg.at[slot, :, pl.ds(0, width)], g_sem.at[slot]),
            pltpu.make_async_copy(wu_hbm.at[:, cols], wu.at[slot, :, pl.ds(0, width)], u_sem.at[slot]),
        )

    def down_copy(c):
        return pltpu.make_async_copy(wd_hbm.at[:, pl.ds(pl.multiple_of(c * OUT_COLS, OUT_COLS), OUT_COLS)], wd.at[c], wd_sem.at[c])

    for i in range(FF_SLOTS):
        for copy in ff_copies(i):
            copy.start()
    for c in range(outs):
        down_copy(c).start()

    pl.semaphore_wait(barrier, n)

    side = round(n ** (1 / 3))
    xs = [lax.rem(lax.rem(me, side) + d, side) for d in range(side)]
    ys = [lax.rem(lax.rem(me // side, side) + d, side) * side for d in range(side)]
    zs = [lax.rem(me // (side * side) + d, side) * (side * side) for d in range(side)]
    hops = lambda o: sum(min(d, side - d) for d in o)
    offsets = sorted(itertools.product(range(side), repeat=3), key=hops, reverse=True)[:-1]
    peers = [xs[a] + ys[b] + zs[c] for a, b, c in offsets]

    def send_part(peer):
        pltpu.make_async_remote_copy(mix_ref.at[peer], got_mix.at[me], mix_send, mix_recv, device_id={'sp': peer}, device_id_type=MESH).start()
        pltpu.make_async_remote_copy(stats_ref.at[peer // per_row], got_stats.at[me], st_send, st_recv, device_id={'sp': peer}, device_id_type=MESH).start()

    for peer in peers:
        send_part(peer)
    got_mix[me] = mix_ref[me]
    got_stats[me] = stats_ref[me // per_row]

    def bulk(ref, send, recv):
        span = ref.at[pl.ds(0, n - 1)]
        return pltpu.make_async_remote_copy(span, span, send, recv, device_id={'tp': partner}, device_id_type=MESH)

    bulk(got_stats, st_send, st_recv).wait_recv()
    flipped[...] = got_stats[:, 0, :].T
    first = pl.multiple_of(lax.rem(me, per_row) * repeat, repeat)
    tops = flipped[pl.ds(first, repeat), :]
    totals = flipped[pl.ds(pl.multiple_of(per_row * repeat + first, repeat), repeat), :]
    factor = jnp.exp(tops - jnp.max(tops, axis=-1, keepdims=True))
    total = jnp.sum(factor * totals, axis=-1, keepdims=True)
    bulk(got_mix, mix_send, mix_recv).wait_recv()
    lanes = 4
    sums = [factor[:, s:s + 1] * got_mix[s] for s in range(lanes)]
    for s in range(lanes, n):
        sums[s % lanes] = sums[s % lanes] + factor[:, s:s + 1] * got_mix[s]
    mixed = (sums[0] + sums[1]) + (sums[2] + sums[3])
    row = (mixed / total).astype(BF16).astype(F32)
    own[...] = row
    gathered[me] = row

    def send_own(peer):
        pltpu.make_async_remote_copy(own, gathered.at[me], own_send, own_recv, device_id={'sp': peer}, device_id_type=MESH).start()

    for peer in peers:
        send_own(peer)
    wo_copy.wait()
    bulk(gathered, own_send, own_recv).wait_recv()
    attended = jnp.concatenate([gathered[:, h, :] for h in range(repeat)], axis=-1).astype(BF16)

    def exchange(mine, theirs, send, recv, c):
        return pltpu.make_async_remote_copy(mine.at[c], theirs.at[c], send.at[c], recv.at[c], device_id={'tp': partner}, device_id_type=MESH)

    for c in range(outs):
        sent[c] = dot(attended, wo[:, c * OUT_COLS:(c + 1) * OUT_COLS])
        exchange(sent, other, o_send, o_recv, c).start()
    for copy in small:
        copy.wait()
    for c in range(outs):
        exchange(sent, other, o_send, o_recv, c).wait_recv()
        cols = slice(c * OUT_COLS, (c + 1) * OUT_COLS)
        mid = (hidden_ref[:, cols].astype(F32) + (sent[c] + other[c])).astype(BF16)
        mid_ref[:, cols] = mid
    normed_ref[0:rows] = rms_norm(mid_ref[...].astype(F32), gain_ref[...].astype(F32)[None, :])

    normed_ref[rows:] = jnp.zeros((PAD_ROWS - rows, normed_ref.shape[1]), BF16)
    act[rows:] = jnp.zeros((PAD_ROWS - rows, act.shape[1]), BF16)

    def inner_step(slot, start, width):
        normed = normed_ref[...]
        gate = dot(normed, wg[slot, :, :width])[:rows]
        up = dot(normed, wu[slot, :, :width])[:rows]
        act[0:rows, pl.ds(start, width)] = (jax.nn.silu(gate) * up).astype(BF16)

    def ff_step(i, carry):
        for copy in ff_copies(i):
            copy.wait()
        slot = lax.rem(i, FF_SLOTS)
        inner_step(slot, pl.multiple_of(i * FF_COLS, FF_COLS), FF_COLS)

        @pl.when(i + FF_SLOTS < full)
        def _():
            for copy in ff_copies(i + FF_SLOTS):
                copy.start()

        if tail:
            @pl.when(i + FF_SLOTS == full)
            def _():
                for copy in ff_copies(full, tail):
                    copy.start()
        return carry

    lax.fori_loop(0, full, ff_step, 0)
    if tail:
        for copy in ff_copies(full, tail):
            copy.wait()
        inner_step(full % FF_SLOTS, full * FF_COLS, tail)

    def down_step(c, carry):
        down_copy(c).wait()
        sent2[c] = dot(act[...], wd[c])[:rows]
        exchange(sent2, other2, d_send, d_recv, c).start()
        return carry

    lax.fori_loop(0, outs, down_step, 0)
    for c in range(outs):
        exchange(sent2, other2, d_send, d_recv, c).wait_recv()
        cols = slice(c * OUT_COLS, (c + 1) * OUT_COLS)
        out_ref[:, cols] = (mid_ref[:, cols].astype(F32) + (sent2[c] + other2[c])).astype(BF16)

    bulk(got_mix, mix_send, mix_recv).wait_send()
    bulk(got_stats, st_send, st_recv).wait_send()
    bulk(gathered, own_send, own_recv).wait_send()
    for c in range(outs):
        exchange(sent, other, o_send, o_recv, c).wait_send()
        exchange(sent2, other2, d_send, d_recv, c).wait_send()


def merge(hidden, mix, stats, gain, w_o, w_gate, w_up, w_down):
    rows, repeat, head_dim = mix.shape
    width = w_o.shape[1]
    inner = w_gate.shape[1]
    outs = width // OUT_COLS
    whole = pl.BlockSpec(memory_space=pltpu.VMEM)
    raw = pl.BlockSpec(memory_space=pltpu.HBM)
    dma = pltpu.SemaphoreType.DMA
    return pl.pallas_call(
        merge_kernel,
        name='merge',
        out_shape=pltpu.VMEM(hidden.shape, BF16),
        in_specs=[raw, whole, whole, raw, raw, raw, raw, raw],
        out_specs=whole,
        scratch_shapes=[
            pltpu.VMEM(hidden.shape, BF16),
            pltpu.VMEM(gain.shape, BF16),
            pltpu.VMEM(mix.shape, F32),
            pltpu.VMEM((rows, 1, 128), F32),
            pltpu.VMEM((128, rows), F32),
            pltpu.VMEM((repeat, head_dim), F32),
            pltpu.VMEM(mix.shape, F32),
            pltpu.VMEM(w_o.shape, BF16),
            pltpu.VMEM((FF_SLOTS, width, FF_COLS), BF16),
            pltpu.VMEM((FF_SLOTS, width, FF_COLS), BF16),
            pltpu.VMEM((outs, inner, OUT_COLS), BF16),
            pltpu.VMEM((outs, rows, OUT_COLS), F32),
            pltpu.VMEM((outs, rows, OUT_COLS), F32),
            pltpu.VMEM((rows, width), BF16),
            pltpu.VMEM((PAD_ROWS, width), BF16),
            pltpu.VMEM((PAD_ROWS, inner), BF16),
            pltpu.VMEM((outs, rows, OUT_COLS), F32),
            pltpu.VMEM((outs, rows, OUT_COLS), F32),
            dma, dma, dma, dma, dma, dma,
            dma((outs,)), dma((outs,)), dma((outs,)), dma((outs,)),
            dma((2,)), dma, dma((FF_SLOTS,)), dma((FF_SLOTS,)), dma((outs,)),
        ],
        compiler_params=pltpu.CompilerParams(collective_id=0, has_side_effects=True, vmem_limit_bytes=58 << 20),
    )(*stay(hidden), *stay(mix, stats, space=pltpu.VMEM), *stay(gain, w_o, w_gate, w_up, w_down))


def solution(mesh):
    cache_spec = P('dp', 'tp', 'sp', None)
    row_spec = P('dp', None)
    col_spec = P(None, 'tp')
    inner_spec = P('tp', None)
    gain_spec = P(None)

    def local_step(hidden, seq_lens, k_cache, v_cache, attn_norm, w_q, w_k, w_v, w_o, mlp_norm, w_gate, w_up, w_down):
        shape = k_cache.shape
        flat = (shape[0] * shape[1], shape[2], shape[3])
        k_out, v_out, mix, stats = attention(hidden, seq_lens, attn_norm, w_q, w_k, w_v, k_cache.reshape(flat), v_cache.reshape(flat))
        hidden_out = merge(hidden, mix, stats, mlp_norm, w_o, w_gate, w_up, w_down)
        return hidden_out, k_out.reshape(shape), v_out.reshape(shape)

    return jax.shard_map(local_step, mesh=mesh, in_specs=(row_spec, P('dp'), cache_spec, cache_spec, gain_spec, col_spec, col_spec, col_spec, inner_spec, gain_spec, col_spec, col_spec, inner_spec), out_specs=(row_spec, cache_spec, cache_spec), check_vma=False)
```

```python
import itertools

import jax
import jax.numpy as jnp
from jax import lax
from jax.experimental import pallas as pl
from jax.experimental.pallas import tpu as pltpu
from jax.sharding import PartitionSpec as P

NORM_EPS = 1e-6
MESH = pl.DeviceIdType.MESH
F32 = jnp.float32
BF16 = jnp.bfloat16
SEQ_CHUNKS = 4
PAD_ROWS = 128
FF_COLS = 512
FF_SLOTS = 6
OUT_COLS = 512


def rms_norm(wide, gain):
    scaled = wide * lax.rsqrt(jnp.mean(wide * wide, axis=-1, keepdims=True) + NORM_EPS)
    return (scaled * gain).astype(BF16)


def dot(a, b):
    return jnp.dot(a, b, preferred_element_type=F32)


def stay(*arrays, space=pltpu.HBM):
    return [pltpu.with_memory_space_constraint(x, space) for x in arrays]


def layer_kernel(lens_hbm, hidden_hbm, gain_hbm, gain2_hbm, wq_hbm, wk_hbm, wv_hbm, k_hbm, v_hbm, wo_hbm, wg_hbm, wu_hbm, wd_hbm,
                 out_ref, kbuf, vbuf,
                 lens_ref, hidden_ref, gain_ref, gain2_ref, wkv, query, new_rows, new_scores, scores, probs, mix_ref, stats_ref,
                 got_mix, got_stats, flipped, own, gathered, wo, wg, wu, wd, sent, other, mid_ref, normed_ref, act, sent2, other2,
                 mix_send, mix_recv, st_send, st_recv, own_send, own_recv, o_send, o_recv, d_send, d_recv,
                 small_sem, w_sem, q_sem, k_sem, v_sem, wo_sem, g_sem, u_sem, wd_sem):
    rows, block_len, head_dim = kbuf.shape
    repeat = mix_ref.shape[1]
    n = rows
    me = lax.axis_index('sp')
    partner = 1 - lax.axis_index('tp')
    base = me * block_len
    scale = head_dim ** -0.5
    per = rows // SEQ_CHUNKS
    inner = wg_hbm.shape[1]
    full = inner // FF_COLS
    tail = inner - full * FF_COLS
    outs = wo_hbm.shape[1] // OUT_COLS
    per_row = 128 // (2 * repeat)

    small = [pltpu.make_async_copy(src, dst, small_sem.at[i]) for i, (src, dst) in enumerate(
        ((hidden_hbm, hidden_ref), (gain_hbm, gain_ref), (lens_hbm, lens_ref), (gain2_hbm, gain2_ref)))]
    for copy in small:
        copy.start()

    kv_copies = [pltpu.make_async_copy(src, wkv.at[:, pl.ds(i * head_dim, head_dim)], w_sem.at[i]) for i, src in enumerate((wk_hbm, wv_hbm))]
    for copy in kv_copies:
        copy.start()
    last = FF_SLOTS - 1
    halves = (wg.at[last], wu.at[last])
    q_copies = [pltpu.make_async_copy(wq_hbm.at[:, pl.ds(i * FF_COLS, FF_COLS)], half, q_sem.at[i]) for i, half in enumerate(halves)]
    for copy in q_copies:
        copy.start()

    def cache_copy(hbm, buf, sems, c):
        part = pl.ds(c * per, per)
        return pltpu.make_async_copy(hbm.at[part], buf.at[part], sems.at[c])

    for c in range(SEQ_CHUNKS):
        cache_copy(k_hbm, kbuf, k_sem, c).start()
    for c in range(SEQ_CHUNKS):
        cache_copy(v_hbm, vbuf, v_sem, c).start()

    barrier = pltpu.get_barrier_semaphore()
    side = round(n ** (1 / 3))
    xs = [lax.rem(lax.rem(me, side) + d, side) for d in range(side)]
    ys = [lax.rem(lax.rem(me // side, side) + d, side) * side for d in range(side)]
    zs = [lax.rem(me // (side * side) + d, side) * (side * side) for d in range(side)]
    hops = lambda o: sum(min(d, side - d) for d in o)
    offsets = sorted(itertools.product(range(side), repeat=3), key=hops, reverse=True)[:-1]
    peers = [xs[a] + ys[b] + zs[c] for a, b, c in offsets]
    for peer in peers:
        pl.semaphore_signal(barrier, inc=1, device_id={'sp': peer}, device_id_type=MESH)
    pl.semaphore_signal(barrier, inc=1, device_id={'tp': partner}, device_id_type=MESH)

    wo_copy = pltpu.make_async_copy(wo_hbm, wo, wo_sem)
    wo_copy.start()

    def ff_copies(i, width=FF_COLS):
        slot = lax.rem(i, FF_SLOTS) if not isinstance(i, int) else i % FF_SLOTS
        start = i * FF_COLS if isinstance(i, int) else pl.multiple_of(i * FF_COLS, FF_COLS)
        cols = pl.ds(start, width)
        return (
            pltpu.make_async_copy(wg_hbm.at[:, cols], wg.at[slot, :, pl.ds(0, width)], g_sem.at[slot]),
            pltpu.make_async_copy(wu_hbm.at[:, cols], wu.at[slot, :, pl.ds(0, width)], u_sem.at[slot]),
        )

    def down_copy(c):
        return pltpu.make_async_copy(wd_hbm.at[:, pl.ds(pl.multiple_of(c * OUT_COLS, OUT_COLS), OUT_COLS)], wd.at[c], wd_sem.at[c])

    for i in range(last):
        for copy in ff_copies(i):
            copy.start()

    normed_ref[rows:] = jnp.zeros((PAD_ROWS - rows, normed_ref.shape[1]), BF16)
    act[rows:] = jnp.zeros((PAD_ROWS - rows, act.shape[1]), BF16)
    for copy in small[:3]:
        copy.wait()
    normed_ref[0:rows] = rms_norm(hidden_ref[...].astype(F32), gain_ref[...].astype(F32)[None, :])
    for copy in kv_copies:
        copy.wait()
    new_rows[...] = dot(normed_ref[...], wkv[...])[:rows].astype(BF16).astype(F32)
    per_half = FF_COLS // head_dim
    for i, half in enumerate(halves):
        q_copies[i].wait()
        part = dot(normed_ref[...], half[...])[:rows].astype(BF16).astype(F32)
        for h in range(per_half):
            query[:, i * per_half + h, :] = part[:, h * head_dim:(h + 1) * head_dim]
    for copy in ff_copies(last):
        copy.start()
    for c in range(outs):
        down_copy(c).start()

    group = 128 // repeat
    for c in range(rows // group):
        part = slice(c * group, (c + 1) * group)
        hit = jnp.sum(query[part] * new_rows[part, :head_dim][:, None, :], axis=-1, keepdims=True) * scale
        new_scores[part] = jnp.broadcast_to(hit, (group, repeat, block_len))

    lanes = lax.broadcasted_iota(jnp.int32, (repeat, block_len), 1)

    def score_chunk(c):
        cache_copy(k_hbm, kbuf, k_sem, c).wait()
        for b in range(c * per, (c + 1) * per):
            slot = lens_ref[b] - base
            raw = lax.dot_general(query[b].astype(BF16), kbuf[b], (((1,), (1,)), ((), ())), preferred_element_type=F32)
            fresh = jnp.where(lanes == slot, new_scores[b], -jnp.inf)
            scores[b] = jnp.where(lanes < slot, raw * scale, fresh)

    for c in range(SEQ_CHUNKS):
        score_chunk(c)

    pairs = lax.broadcasted_iota(jnp.int32, (128, block_len), 1)
    half_pairs = group // 2 * repeat
    low = lax.broadcasted_iota(jnp.int32, (1, 128), 1) < half_pairs
    for c in range(rows // group):
        part = slice(c * group, (c + 1) * group)
        s = scores[part].reshape(128, block_len)
        top = jnp.max(s, axis=-1, keepdims=True)
        p = jnp.where(s > -jnp.inf, jnp.exp(s - top), 0.0)
        total = jnp.sum(p, axis=-1, keepdims=True)
        probs[part] = p.reshape(group, repeat, block_len)
        turned = jnp.where(pairs == 0, top, jnp.where(pairs == 1, total, 0.0)).T
        m_row, l_row = turned[0:1], turned[1:2]
        stats_ref[2 * c] = jnp.where(low, m_row, pltpu.roll(l_row, half_pairs, 1))
        stats_ref[2 * c + 1] = jnp.where(low, pltpu.roll(m_row, half_pairs, 1), l_row)

    def mix_chunk(c):
        cache_copy(v_hbm, vbuf, v_sem, c).wait()
        for b in range(c * per, (c + 1) * per):
            here = lanes == lens_ref[b] - base
            p = probs[b].astype(BF16).astype(F32)
            fresh = jnp.sum(jnp.where(here, p, 0.0), axis=-1, keepdims=True)
            mix_ref[b] = dot(jnp.where(here, 0.0, p).astype(BF16), vbuf[b]) + fresh * new_rows[b:b + 1, head_dim:]

    for c in range(SEQ_CHUNKS):
        mix_chunk(c)

    pl.semaphore_wait(barrier, n)
    for peer in peers:
        pltpu.make_async_remote_copy(mix_ref.at[peer], got_mix.at[me], mix_send, mix_recv, device_id={'sp': peer}, device_id_type=MESH).start()
        pltpu.make_async_remote_copy(stats_ref.at[peer // per_row], got_stats.at[me], st_send, st_recv, device_id={'sp': peer}, device_id_type=MESH).start()
    got_mix[me] = mix_ref[me]
    got_stats[me] = stats_ref[me // per_row]

    tile = lax.broadcasted_iota(jnp.int32, (block_len, head_dim), 0)

    def insert(b, carry):
        here = tile == lens_ref[b] - base
        new = new_rows[pl.ds(b, 1), :].astype(BF16)
        kbuf[b] = jnp.where(here, jnp.broadcast_to(new[:, :head_dim], here.shape), kbuf[b])
        vbuf[b] = jnp.where(here, jnp.broadcast_to(new[:, head_dim:], here.shape), vbuf[b])
        return carry

    lax.fori_loop(0, rows, insert, 0)

    def bulk(ref, send, recv):
        span = ref.at[pl.ds(0, n - 1)]
        return pltpu.make_async_remote_copy(span, span, send, recv, device_id={'tp': partner}, device_id_type=MESH)

    bulk(got_stats, st_send, st_recv).wait_recv()
    flipped[...] = got_stats[:, 0, :].T
    first = pl.multiple_of(lax.rem(me, per_row) * repeat, repeat)
    tops = flipped[pl.ds(first, repeat), :]
    totals = flipped[pl.ds(pl.multiple_of(per_row * repeat + first, repeat), repeat), :]
    factor = jnp.exp(tops - jnp.max(tops, axis=-1, keepdims=True))
    total = jnp.sum(factor * totals, axis=-1, keepdims=True)
    bulk(got_mix, mix_send, mix_recv).wait_recv()
    ways = 4
    sums = [factor[:, s:s + 1] * got_mix[s] for s in range(ways)]
    for s in range(ways, n):
        sums[s % ways] = sums[s % ways] + factor[:, s:s + 1] * got_mix[s]
    mixed = (sums[0] + sums[1]) + (sums[2] + sums[3])
    row = (mixed / total).astype(BF16).astype(F32)
    own[...] = row
    gathered[me] = row
    for peer in peers:
        pltpu.make_async_remote_copy(own, gathered.at[me], own_send, own_recv, device_id={'sp': peer}, device_id_type=MESH).start()
    small[3].wait()
    wo_copy.wait()
    bulk(gathered, own_send, own_recv).wait_recv()
    attended = jnp.concatenate([gathered[:, h, :] for h in range(repeat)], axis=-1).astype(BF16)

    def exchange(mine, theirs, send, recv, c):
        return pltpu.make_async_remote_copy(mine.at[c], theirs.at[c], send.at[c], recv.at[c], device_id={'tp': partner}, device_id_type=MESH)

    for c in range(outs):
        sent[c] = dot(attended, wo[:, c * OUT_COLS:(c + 1) * OUT_COLS])
        exchange(sent, other, o_send, o_recv, c).start()
    for c in range(outs):
        exchange(sent, other, o_send, o_recv, c).wait_recv()
        cols = slice(c * OUT_COLS, (c + 1) * OUT_COLS)
        mid_ref[:, cols] = (hidden_ref[:, cols].astype(F32) + (sent[c] + other[c])).astype(BF16)
    normed_ref[0:rows] = rms_norm(mid_ref[...].astype(F32), gain2_ref[...].astype(F32)[None, :])

    def inner_step(slot, start, width):
        normed = normed_ref[...]
        gate = dot(normed, wg[slot, :, :width])[:rows]
        up = dot(normed, wu[slot, :, :width])[:rows]
        act[0:rows, pl.ds(start, width)] = (jax.nn.silu(gate) * up).astype(BF16)

    def ff_step(i, carry):
        for copy in ff_copies(i):
            copy.wait()
        inner_step(lax.rem(i, FF_SLOTS), pl.multiple_of(i * FF_COLS, FF_COLS), FF_COLS)

        @pl.when(i + FF_SLOTS < full)
        def _():
            for copy in ff_copies(i + FF_SLOTS):
                copy.start()

        if tail:
            @pl.when(i + FF_SLOTS == full)
            def _():
                for copy in ff_copies(full, tail):
                    copy.start()
        return carry

    lax.fori_loop(0, full, ff_step, 0)
    if tail:
        for copy in ff_copies(full, tail):
            copy.wait()
        inner_step(full % FF_SLOTS, full * FF_COLS, tail)

    def down_step(c, carry):
        down_copy(c).wait()
        sent2[c] = dot(act[...], wd[c])[:rows]
        exchange(sent2, other2, d_send, d_recv, c).start()
        return carry

    lax.fori_loop(0, outs, down_step, 0)
    for c in range(outs):
        exchange(sent2, other2, d_send, d_recv, c).wait_recv()
        cols = slice(c * OUT_COLS, (c + 1) * OUT_COLS)
        out_ref[:, cols] = (mid_ref[:, cols].astype(F32) + (sent2[c] + other2[c])).astype(BF16)

    bulk(got_mix, mix_send, mix_recv).wait_send()
    bulk(got_stats, st_send, st_recv).wait_send()
    bulk(gathered, own_send, own_recv).wait_send()
    for c in range(outs):
        exchange(sent, other, o_send, o_recv, c).wait_send()
        exchange(sent2, other2, d_send, d_recv, c).wait_send()


def layer(seq_lens, hidden, gain, gain2, w_q, w_k, w_v, k_cache, v_cache, w_o, w_gate, w_up, w_down):
    rows, block_len, head_dim = k_cache.shape
    repeat = w_q.shape[1] // head_dim
    width = w_o.shape[1]
    inner = w_gate.shape[1]
    outs = width // OUT_COLS
    assert w_q.shape[1] == 2 * FF_COLS
    raw = pl.BlockSpec(memory_space=pltpu.HBM)
    whole = pl.BlockSpec(memory_space=pltpu.VMEM)
    dma = pltpu.SemaphoreType.DMA
    heads = (rows, repeat, head_dim)
    return pl.pallas_call(
        layer_kernel,
        name='layer',
        out_shape=(pltpu.VMEM(hidden.shape, BF16), pltpu.VMEM(k_cache.shape, BF16), pltpu.VMEM(v_cache.shape, BF16)),
        in_specs=[raw] * 13,
        out_specs=(whole, whole, whole),
        scratch_shapes=[
            pltpu.SMEM(seq_lens.shape, jnp.int32),
            pltpu.VMEM(hidden.shape, BF16),
            pltpu.VMEM(gain.shape, BF16),
            pltpu.VMEM(gain2.shape, BF16),
            pltpu.VMEM((width, 2 * head_dim), BF16),
            pltpu.VMEM(heads, F32),
            pltpu.VMEM((rows, 2 * head_dim), F32),
            pltpu.VMEM((rows, repeat, block_len), F32),
            pltpu.VMEM((rows, repeat, block_len), F32),
            pltpu.VMEM((rows, repeat, block_len), F32),
            pltpu.VMEM(heads, F32),
            pltpu.VMEM((2 * rows * repeat // 128, 1, 128), F32),
            pltpu.VMEM(heads, F32),
            pltpu.VMEM((rows, 1, 128), F32),
            pltpu.VMEM((128, rows), F32),
            pltpu.VMEM((repeat, head_dim), F32),
            pltpu.VMEM(heads, F32),
            pltpu.VMEM(w_o.shape, BF16),
            pltpu.VMEM((FF_SLOTS, width, FF_COLS), BF16),
            pltpu.VMEM((FF_SLOTS, width, FF_COLS), BF16),
            pltpu.VMEM((outs, inner, OUT_COLS), BF16),
            pltpu.VMEM((outs, rows, OUT_COLS), F32),
            pltpu.VMEM((outs, rows, OUT_COLS), F32),
            pltpu.VMEM((rows, width), BF16),
            pltpu.VMEM((PAD_ROWS, width), BF16),
            pltpu.VMEM((PAD_ROWS, inner), BF16),
            pltpu.VMEM((outs, rows, OUT_COLS), F32),
            pltpu.VMEM((outs, rows, OUT_COLS), F32),
            dma, dma, dma, dma, dma, dma,
            dma((outs,)), dma((outs,)), dma((outs,)), dma((outs,)),
            dma((4,)), dma((2,)), dma((2,)), dma((SEQ_CHUNKS,)), dma((SEQ_CHUNKS,)),
            dma, dma((FF_SLOTS,)), dma((FF_SLOTS,)), dma((outs,)),
        ],
        compiler_params=pltpu.CompilerParams(collective_id=0, has_side_effects=True, vmem_limit_bytes=59 << 20),
    )(*stay(seq_lens, hidden, gain, gain2, w_q, w_k, w_v, k_cache, v_cache, w_o, w_gate, w_up, w_down))


def write_kernel(*refs):
    count = len(refs) // 2
    sems = refs[-1]
    copies = [pltpu.make_async_copy(refs[i], refs[count + i], sems.at[i]) for i in range(count)]
    for copy in copies:
        copy.start()
    for copy in copies:
        copy.wait()


def write(*arrays):
    return pl.pallas_call(
        write_kernel,
        name='write',
        out_shape=tuple(pltpu.HBM(x.shape, x.dtype) for x in arrays),
        in_specs=[pl.BlockSpec(memory_space=pltpu.VMEM)] * len(arrays),
        out_specs=tuple(pl.BlockSpec(memory_space=pltpu.HBM) for _ in arrays),
        scratch_shapes=[pltpu.SemaphoreType.DMA((len(arrays),))],
        compiler_params=pltpu.CompilerParams(vmem_limit_bytes=4 << 20),
    )(*stay(*arrays, space=pltpu.VMEM))


def solution(mesh):
    cache_spec = P('dp', 'tp', 'sp', None)
    row_spec = P('dp', None)
    col_spec = P(None, 'tp')
    inner_spec = P('tp', None)
    gain_spec = P(None)

    def local_step(hidden, seq_lens, k_cache, v_cache, attn_norm, w_q, w_k, w_v, w_o, mlp_norm, w_gate, w_up, w_down):
        shape = k_cache.shape
        flat = (shape[0] * shape[1], shape[2], shape[3])
        parts = layer(seq_lens, hidden, attn_norm, mlp_norm, w_q, w_k, w_v, k_cache.reshape(flat), v_cache.reshape(flat), w_o, w_gate, w_up, w_down)
        hidden_out, k_out, v_out = write(*parts)
        return hidden_out, k_out.reshape(shape), v_out.reshape(shape)

    return jax.shard_map(local_step, mesh=mesh, in_specs=(row_spec, P('dp'), cache_spec, cache_spec, gain_spec, col_spec, col_spec, col_spec, inner_spec, gain_spec, col_spec, col_spec, inner_spec), out_specs=(row_spec, cache_spec, cache_spec), check_vma=False)
```

```python
import itertools

import jax
import jax.numpy as jnp
from jax import lax
from jax.experimental import pallas as pl
from jax.experimental.pallas import tpu as pltpu
from jax.sharding import PartitionSpec as P

NORM_EPS = 1e-6
MESH = pl.DeviceIdType.MESH
F32 = jnp.float32
BF16 = jnp.bfloat16
SEQ_CHUNKS = 4
PAD_ROWS = 128
FF_COLS = 512
FF_SLOTS = 7
OUT_COLS = 512
FF_GROUPS = ((0, 6), (6, 8), (8, 10), (10, 11))


def rms_norm(wide, gain):
    scaled = wide * lax.rsqrt(jnp.mean(wide * wide, axis=-1, keepdims=True) + NORM_EPS)
    return (scaled * gain).astype(BF16)


def dot(a, b):
    return jnp.dot(a, b, preferred_element_type=F32)


def stay(*arrays, space=pltpu.HBM):
    return [pltpu.with_memory_space_constraint(x, space) for x in arrays]


def layer_kernel(lens_hbm, hidden_hbm, gain_hbm, gain2_hbm, wq_hbm, wk_hbm, wv_hbm, k_hbm, v_hbm, wo_hbm, wg_hbm, wu_hbm, wd_hbm,
                 out_ref, kbuf, vbuf,
                 lens_ref, hidden_ref, gain_ref, gain2_ref, query, new_rows, new_scores, scores, probs, mix_ref, stats_ref,
                 got_mix, got_stats, flipped, own, gathered, wg, wu, wd, sent, other, mid_ref, normed_ref, act, sent2, other2,
                 mix_send, mix_recv, st_send, st_recv, own_send, own_recv, o_send, o_recv, d_send, d_recv,
                 small_sem, w_sem, q_sem, k_sem, v_sem, wo_sem, g_sem, u_sem, wd_sem):
    rows, block_len, head_dim = kbuf.shape
    repeat = mix_ref.shape[1]
    n = rows
    me = lax.axis_index('sp')
    partner = 1 - lax.axis_index('tp')
    base = me * block_len
    scale = head_dim ** -0.5
    per = rows // SEQ_CHUNKS
    inner = wg_hbm.shape[1]
    full = inner // FF_COLS
    tail = inner - full * FF_COLS
    outs = wo_hbm.shape[1] // OUT_COLS
    per_row = 128 // (2 * repeat)

    small = [pltpu.make_async_copy(src, dst, small_sem.at[i]) for i, (src, dst) in enumerate(
        ((hidden_hbm, hidden_ref), (gain_hbm, gain_ref), (lens_hbm, lens_ref), (gain2_hbm, gain2_ref)))]
    for copy in small:
        copy.start()

    wkv = wd.at[outs - 1, pl.ds(0, wk_hbm.shape[0]), pl.ds(0, 2 * head_dim)]
    kv_copies = [pltpu.make_async_copy(src, wd.at[outs - 1, pl.ds(0, wk_hbm.shape[0])].at[:, pl.ds(i * head_dim, head_dim)], w_sem.at[i]) for i, src in enumerate((wk_hbm, wv_hbm))]
    for copy in kv_copies:
        copy.start()
    q_slot, o_slot = FF_SLOTS - 2, FF_SLOTS - 1
    halves = (wg.at[q_slot], wu.at[q_slot])
    q_copies = [pltpu.make_async_copy(wq_hbm.at[:, pl.ds(i * FF_COLS, FF_COLS)], half, q_sem.at[i]) for i, half in enumerate(halves)]
    for copy in q_copies:
        copy.start()

    def cache_copy(hbm, buf, sems, c):
        part = pl.ds(c * per, per)
        return pltpu.make_async_copy(hbm.at[part], buf.at[part], sems.at[c])

    for c in range(SEQ_CHUNKS):
        cache_copy(k_hbm, kbuf, k_sem, c).start()
    for c in range(SEQ_CHUNKS):
        cache_copy(v_hbm, vbuf, v_sem, c).start()

    barrier = pltpu.get_barrier_semaphore()
    side = round(n ** (1 / 3))
    xs = [lax.rem(lax.rem(me, side) + d, side) for d in range(side)]
    ys = [lax.rem(lax.rem(me // side, side) + d, side) * side for d in range(side)]
    zs = [lax.rem(me // (side * side) + d, side) * (side * side) for d in range(side)]
    hops = lambda o: sum(min(d, side - d) for d in o)
    offsets = sorted(itertools.product(range(side), repeat=3), key=hops, reverse=True)[:-1]
    peers = [xs[a] + ys[b] + zs[c] for a, b, c in offsets]
    for peer in peers:
        pl.semaphore_signal(barrier, inc=1, device_id={'sp': peer}, device_id_type=MESH)
    pl.semaphore_signal(barrier, inc=1, device_id={'tp': partner}, device_id_type=MESH)

    depth = wo_hbm.shape[0]
    o_parts = [(wg, wu)[c // 2].at[o_slot, pl.ds(c % 2 * depth, depth)] for c in range(outs)]
    o_copies = [pltpu.make_async_copy(wo_hbm.at[:, pl.ds(c * OUT_COLS, OUT_COLS)], part, wo_sem.at[c]) for c, part in enumerate(o_parts)]

    chunks = full + (tail > 0)

    def ff_copies(i):
        slot, width = i % FF_SLOTS, min(FF_COLS, inner - i * FF_COLS)
        cols = pl.ds(i * FF_COLS, width)
        return (
            pltpu.make_async_copy(wg_hbm.at[:, cols], wg.at[slot, :, pl.ds(0, width)], g_sem.at[slot]),
            pltpu.make_async_copy(wu_hbm.at[:, cols], wu.at[slot, :, pl.ds(0, width)], u_sem.at[slot]),
        )

    def down_copy(c):
        return pltpu.make_async_copy(wd_hbm.at[:, pl.ds(c * OUT_COLS, OUT_COLS)], wd.at[c], wd_sem.at[c])

    def start(copies):
        for copy in copies:
            copy.start()

    def wait(copies):
        for copy in copies:
            copy.wait()

    normed_ref[rows:] = jnp.zeros((PAD_ROWS - rows, normed_ref.shape[1]), BF16)
    act[rows:] = jnp.zeros((PAD_ROWS - rows, act.shape[1]), BF16)
    for copy in small[:3]:
        copy.wait()
    normed_ref[0:rows] = rms_norm(hidden_ref[...].astype(F32), gain_ref[...].astype(F32)[None, :])
    wait(kv_copies)
    wait(q_copies)
    new_rows[...] = dot(normed_ref[...], wkv[...])[:rows].astype(BF16).astype(F32)
    per_half = FF_COLS // head_dim
    for i, half in enumerate(halves):
        part = dot(normed_ref[...], half[...])[:rows].astype(BF16).astype(F32)
        for h in range(per_half):
            query[:, i * per_half + h, :] = part[:, h * head_dim:(h + 1) * head_dim]
    for i in range(q_slot + 1):
        start(ff_copies(i))

    group = 128 // repeat
    for c in range(rows // group):
        part = slice(c * group, (c + 1) * group)
        hit = jnp.sum(query[part] * new_rows[part, :head_dim][:, None, :], axis=-1, keepdims=True) * scale
        new_scores[part] = jnp.broadcast_to(hit, (group, repeat, block_len))

    lanes = lax.broadcasted_iota(jnp.int32, (repeat, block_len), 1)

    def score_chunk(c):
        for b in range(c * per, (c + 1) * per):
            slot = lens_ref[b] - base
            raw = lax.dot_general(query[b].astype(BF16), kbuf[b], (((1,), (1,)), ((), ())), preferred_element_type=F32)
            fresh = jnp.where(lanes == slot, new_scores[b], -jnp.inf)
            scores[b] = jnp.where(lanes < slot, raw * scale, fresh)

    wait([cache_copy(k_hbm, kbuf, k_sem, c) for c in range(SEQ_CHUNKS)])
    wait([cache_copy(v_hbm, vbuf, v_sem, c) for c in range(SEQ_CHUNKS)])
    for c in range(SEQ_CHUNKS):
        score_chunk(c)

    pairs = lax.broadcasted_iota(jnp.int32, (128, block_len), 1)
    half_pairs = group // 2 * repeat
    low = lax.broadcasted_iota(jnp.int32, (1, 128), 1) < half_pairs
    for c in range(rows // group):
        part = slice(c * group, (c + 1) * group)
        s = scores[part].reshape(128, block_len)
        top = jnp.max(s, axis=-1, keepdims=True)
        p = jnp.where(s > -jnp.inf, jnp.exp(s - top), 0.0)
        total = jnp.sum(p, axis=-1, keepdims=True)
        probs[part] = p.reshape(group, repeat, block_len)
        turned = jnp.where(pairs == 0, top, jnp.where(pairs == 1, total, 0.0)).T
        m_row, l_row = turned[0:1], turned[1:2]
        stats_ref[2 * c] = jnp.where(low, m_row, pltpu.roll(l_row, half_pairs, 1))
        stats_ref[2 * c + 1] = jnp.where(low, pltpu.roll(m_row, half_pairs, 1), l_row)

    def mix_chunk(c):
        for b in range(c * per, (c + 1) * per):
            here = lanes == lens_ref[b] - base
            p = probs[b].astype(BF16).astype(F32)
            fresh = jnp.sum(jnp.where(here, p, 0.0), axis=-1, keepdims=True)
            mix_ref[b] = dot(jnp.where(here, 0.0, p).astype(BF16), vbuf[b]) + fresh * new_rows[b:b + 1, head_dim:]

    for c in range(SEQ_CHUNKS):
        mix_chunk(c)

    pl.semaphore_wait(barrier, n)
    for peer in peers:
        pltpu.make_async_remote_copy(mix_ref.at[peer], got_mix.at[me], mix_send, mix_recv, device_id={'sp': peer}, device_id_type=MESH).start()
        pltpu.make_async_remote_copy(stats_ref.at[peer // per_row], got_stats.at[me], st_send, st_recv, device_id={'sp': peer}, device_id_type=MESH).start()
    got_mix[me] = mix_ref[me]
    got_stats[me] = stats_ref[me // per_row]
    start(o_copies)
    start([down_copy(c) for c in range(outs)])

    tile = lax.broadcasted_iota(jnp.int32, (block_len, head_dim), 0)

    def insert(b, carry):
        here = tile == lens_ref[b] - base
        new = new_rows[pl.ds(b, 1), :].astype(BF16)
        kbuf[b] = jnp.where(here, jnp.broadcast_to(new[:, :head_dim], here.shape), kbuf[b])
        vbuf[b] = jnp.where(here, jnp.broadcast_to(new[:, head_dim:], here.shape), vbuf[b])
        return carry

    lax.fori_loop(0, rows, insert, 0)

    def bulk(ref, send, recv):
        span = ref.at[pl.ds(0, n - 1)]
        return pltpu.make_async_remote_copy(span, span, send, recv, device_id={'tp': partner}, device_id_type=MESH)

    bulk(got_stats, st_send, st_recv).wait_recv()
    flipped[...] = got_stats[:, 0, :].T
    first = pl.multiple_of(lax.rem(me, per_row) * repeat, repeat)
    tops = flipped[pl.ds(first, repeat), :]
    totals = flipped[pl.ds(pl.multiple_of(per_row * repeat + first, repeat), repeat), :]
    factor = jnp.exp(tops - jnp.max(tops, axis=-1, keepdims=True))
    total = jnp.sum(factor * totals, axis=-1, keepdims=True)
    bulk(got_mix, mix_send, mix_recv).wait_recv()
    ways = 4
    sums = [factor[:, s:s + 1] * got_mix[s] for s in range(ways)]
    for s in range(ways, n):
        sums[s % ways] = sums[s % ways] + factor[:, s:s + 1] * got_mix[s]
    mixed = (sums[0] + sums[1]) + (sums[2] + sums[3])
    row = (mixed / total).astype(BF16).astype(F32)
    own[...] = row
    gathered[me] = row
    for peer in peers:
        pltpu.make_async_remote_copy(own, gathered.at[me], own_send, own_recv, device_id={'sp': peer}, device_id_type=MESH).start()
    small[3].wait()
    wait(o_copies)
    bulk(gathered, own_send, own_recv).wait_recv()
    attended = jnp.concatenate([gathered[:, h, :] for h in range(repeat)], axis=-1).astype(BF16)
    attended = jnp.concatenate([attended, jnp.zeros((PAD_ROWS - rows, attended.shape[1]), BF16)], axis=0)

    def exchange(mine, theirs, send, recv, c):
        return pltpu.make_async_remote_copy(mine.at[c], theirs.at[c], send.at[c], recv.at[c], device_id={'tp': partner}, device_id_type=MESH)

    for c in range(outs):
        sent[c] = dot(attended, o_parts[c][...])[:rows]
        exchange(sent, other, o_send, o_recv, c).start()
    for i in range(o_slot, FF_SLOTS):
        start(ff_copies(i))
    for c in range(outs):
        exchange(sent, other, o_send, o_recv, c).wait_recv()
        cols = slice(c * OUT_COLS, (c + 1) * OUT_COLS)
        mid_ref[:, cols] = (hidden_ref[:, cols].astype(F32) + (sent[c] + other[c])).astype(BF16)
    normed_ref[0:rows] = rms_norm(mid_ref[...].astype(F32), gain2_ref[...].astype(F32)[None, :])

    def inner_step(i):
        slot, width = i % FF_SLOTS, min(FF_COLS, inner - i * FF_COLS)
        gate = dot(normed_ref[...], wg[slot, :, :width])[:rows]
        up = dot(normed_ref[...], wu[slot, :, :width])[:rows]
        act[0:rows, i * FF_COLS:i * FF_COLS + width] = (jax.nn.silu(gate) * up).astype(BF16)
        if i + FF_SLOTS < chunks:
            start(ff_copies(i + FF_SLOTS))

    for lo, hi in FF_GROUPS:
        for i in range(lo, min(hi, chunks)):
            wait(ff_copies(i))
        for i in range(lo, min(hi, chunks)):
            inner_step(i)

    wait([down_copy(c) for c in range(outs)])
    for c in range(outs):
        sent2[c] = dot(act[...], wd[c])[:rows]
        exchange(sent2, other2, d_send, d_recv, c).start()
    for c in range(outs):
        exchange(sent2, other2, d_send, d_recv, c).wait_recv()
        cols = slice(c * OUT_COLS, (c + 1) * OUT_COLS)
        out_ref[:, cols] = (mid_ref[:, cols].astype(F32) + (sent2[c] + other2[c])).astype(BF16)

    bulk(got_mix, mix_send, mix_recv).wait_send()
    bulk(got_stats, st_send, st_recv).wait_send()
    bulk(gathered, own_send, own_recv).wait_send()
    for c in range(outs):
        exchange(sent, other, o_send, o_recv, c).wait_send()
        exchange(sent2, other2, d_send, d_recv, c).wait_send()


def layer(seq_lens, hidden, gain, gain2, w_q, w_k, w_v, k_cache, v_cache, w_o, w_gate, w_up, w_down):
    rows, block_len, head_dim = k_cache.shape
    repeat = w_q.shape[1] // head_dim
    width = w_o.shape[1]
    inner = w_gate.shape[1]
    outs = width // OUT_COLS
    assert w_q.shape[1] == 2 * FF_COLS
    raw = pl.BlockSpec(memory_space=pltpu.HBM)
    whole = pl.BlockSpec(memory_space=pltpu.VMEM)
    dma = pltpu.SemaphoreType.DMA
    heads = (rows, repeat, head_dim)
    return pl.pallas_call(
        layer_kernel,
        name='layer',
        out_shape=(pltpu.VMEM(hidden.shape, BF16), pltpu.VMEM(k_cache.shape, BF16), pltpu.VMEM(v_cache.shape, BF16)),
        in_specs=[raw] * 13,
        out_specs=(whole, whole, whole),
        scratch_shapes=[
            pltpu.SMEM(seq_lens.shape, jnp.int32),
            pltpu.VMEM(hidden.shape, BF16),
            pltpu.VMEM(gain.shape, BF16),
            pltpu.VMEM(gain2.shape, BF16),
            pltpu.VMEM(heads, F32),
            pltpu.VMEM((rows, 2 * head_dim), F32),
            pltpu.VMEM((rows, repeat, block_len), F32),
            pltpu.VMEM((rows, repeat, block_len), F32),
            pltpu.VMEM((rows, repeat, block_len), F32),
            pltpu.VMEM(heads, F32),
            pltpu.VMEM((2 * rows * repeat // 128, 1, 128), F32),
            pltpu.VMEM(heads, F32),
            pltpu.VMEM((rows, 1, 128), F32),
            pltpu.VMEM((128, rows), F32),
            pltpu.VMEM((repeat, head_dim), F32),
            pltpu.VMEM(heads, F32),
            pltpu.VMEM((FF_SLOTS, width, FF_COLS), BF16),
            pltpu.VMEM((FF_SLOTS, width, FF_COLS), BF16),
            pltpu.VMEM((outs, inner, OUT_COLS), BF16),
            pltpu.VMEM((outs, rows, OUT_COLS), F32),
            pltpu.VMEM((outs, rows, OUT_COLS), F32),
            pltpu.VMEM((rows, width), BF16),
            pltpu.VMEM((PAD_ROWS, width), BF16),
            pltpu.VMEM((PAD_ROWS, inner), BF16),
            pltpu.VMEM((outs, rows, OUT_COLS), F32),
            pltpu.VMEM((outs, rows, OUT_COLS), F32),
            dma, dma, dma, dma, dma, dma,
            dma((outs,)), dma((outs,)), dma((outs,)), dma((outs,)),
            dma((4,)), dma((2,)), dma((2,)), dma((SEQ_CHUNKS,)), dma((SEQ_CHUNKS,)),
            dma((outs,)), dma((FF_SLOTS,)), dma((FF_SLOTS,)), dma((outs,)),
        ],
        compiler_params=pltpu.CompilerParams(collective_id=0, has_side_effects=True, vmem_limit_bytes=59 << 20),
    )(*stay(seq_lens, hidden, gain, gain2, w_q, w_k, w_v, k_cache, v_cache, w_o, w_gate, w_up, w_down))


def write_kernel(*refs):
    count = len(refs) // 2
    sems = refs[-1]
    copies = [pltpu.make_async_copy(refs[i], refs[count + i], sems.at[i]) for i in range(count)]
    for copy in copies:
        copy.start()
    for copy in copies:
        copy.wait()


def write(*arrays):
    return pl.pallas_call(
        write_kernel,
        name='write',
        out_shape=tuple(pltpu.HBM(x.shape, x.dtype) for x in arrays),
        in_specs=[pl.BlockSpec(memory_space=pltpu.VMEM)] * len(arrays),
        out_specs=tuple(pl.BlockSpec(memory_space=pltpu.HBM) for _ in arrays),
        scratch_shapes=[pltpu.SemaphoreType.DMA((len(arrays),))],
        compiler_params=pltpu.CompilerParams(vmem_limit_bytes=4 << 20),
    )(*stay(*arrays, space=pltpu.VMEM))


def solution(mesh):
    cache_spec = P('dp', 'tp', 'sp', None)
    row_spec = P('dp', None)
    col_spec = P(None, 'tp')
    inner_spec = P('tp', None)
    gain_spec = P(None)

    def local_step(hidden, seq_lens, k_cache, v_cache, attn_norm, w_q, w_k, w_v, w_o, mlp_norm, w_gate, w_up, w_down):
        shape = k_cache.shape
        flat = (shape[0] * shape[1], shape[2], shape[3])
        parts = layer(seq_lens, hidden, attn_norm, mlp_norm, w_q, w_k, w_v, k_cache.reshape(flat), v_cache.reshape(flat), w_o, w_gate, w_up, w_down)
        hidden_out, k_out, v_out = write(*parts)
        return hidden_out, k_out.reshape(shape), v_out.reshape(shape)

    return jax.shard_map(local_step, mesh=mesh, in_specs=(row_spec, P('dp'), cache_spec, cache_spec, gain_spec, col_spec, col_spec, col_spec, inner_spec, gain_spec, col_spec, col_spec, inner_spec), out_specs=(row_spec, cache_spec, cache_spec), check_vma=False)
```

```python
import itertools

import jax
import jax.numpy as jnp
from jax import lax
from jax.experimental import pallas as pl
from jax.experimental.pallas import tpu as pltpu
from jax.sharding import PartitionSpec as P

NORM_EPS = 1e-6
MESH = pl.DeviceIdType.MESH
F32 = jnp.float32
BF16 = jnp.bfloat16
SEQ_CHUNKS = 4
PAD_ROWS = 128
FF_COLS = 512
FF_SLOTS = 8
OUT_COLS = 512
FF_GROUPS = ((0, 7), (7, 9), (9, 11))
LAST_SLOT = 3


def rms_norm(wide, gain):
    scaled = wide * lax.rsqrt(jnp.mean(wide * wide, axis=-1, keepdims=True) + NORM_EPS)
    return (scaled * gain).astype(BF16)


def dot(a, b):
    return jnp.dot(a, b, preferred_element_type=F32)


def stay(*arrays, space=pltpu.HBM):
    return [pltpu.with_memory_space_constraint(x, space) for x in arrays]


def layer_kernel(lens_hbm, hidden_hbm, gain_hbm, gain2_hbm, wq_hbm, wk_hbm, wv_hbm, k_hbm, v_hbm, wo_hbm, wg_hbm, wu_hbm, wd_hbm,
                 out_ref, kbuf, vbuf,
                 lens_ref, hidden_ref, gain_ref, gain2_ref, query, new_rows, new_scores, scores, probs, mix_ref, stats_ref,
                 got_mix, got_stats, flipped, own, gathered, wg, wu, wd, sent, other, mid_ref, normed_ref, act, sent2, other2,
                 mix_send, mix_recv, st_send, st_recv, own_send, own_recv, o_send, o_recv, d_send, d_recv,
                 small_sem, w_sem, q_sem, k_sem, v_sem, wo_sem, g_sem, u_sem, wd_sem, last_sem):
    rows, block_len, head_dim = kbuf.shape
    repeat = mix_ref.shape[1]
    n = rows
    me = lax.axis_index('sp')
    partner = 1 - lax.axis_index('tp')
    base = me * block_len
    scale = head_dim ** -0.5
    per = rows // SEQ_CHUNKS
    inner = wg_hbm.shape[1]
    full = inner // FF_COLS
    tail = inner - full * FF_COLS
    outs = wo_hbm.shape[1] // OUT_COLS
    per_row = 128 // (2 * repeat)

    small = [pltpu.make_async_copy(src, dst, small_sem.at[i]) for i, (src, dst) in enumerate(
        ((hidden_hbm, hidden_ref), (gain_hbm, gain_ref), (lens_hbm, lens_ref), (gain2_hbm, gain2_ref)))]
    for copy in small:
        copy.start()

    wkv = wd.at[outs - 2, pl.ds(0, wk_hbm.shape[0]), pl.ds(0, 2 * head_dim)]
    kv_copies = [pltpu.make_async_copy(src, wd.at[outs - 2, pl.ds(0, wk_hbm.shape[0])].at[:, pl.ds(i * head_dim, head_dim)], w_sem.at[i]) for i, src in enumerate((wk_hbm, wv_hbm))]
    for copy in kv_copies:
        copy.start()
    q_slot, o_slot = FF_SLOTS - 2, FF_SLOTS - 1
    halves = (wg.at[q_slot], wu.at[q_slot])
    q_copies = [pltpu.make_async_copy(wq_hbm.at[:, pl.ds(i * FF_COLS, FF_COLS)], half, q_sem.at[i]) for i, half in enumerate(halves)]
    for copy in q_copies:
        copy.start()

    def cache_copy(hbm, buf, sems, c):
        part = pl.ds(c * per, per)
        return pltpu.make_async_copy(hbm.at[part], buf.at[part], sems.at[c])

    barrier = pltpu.get_barrier_semaphore()
    side = round(n ** (1 / 3))
    xs = [lax.rem(lax.rem(me, side) + d, side) for d in range(side)]
    ys = [lax.rem(lax.rem(me // side, side) + d, side) * side for d in range(side)]
    zs = [lax.rem(me // (side * side) + d, side) * (side * side) for d in range(side)]
    hops = lambda o: sum(min(d, side - d) for d in o)
    offsets = sorted(itertools.product(range(side), repeat=3), key=hops, reverse=True)[:-1]
    peers = [xs[a] + ys[b] + zs[c] for a, b, c in offsets]
    for peer in peers:
        pl.semaphore_signal(barrier, inc=1, device_id={'sp': peer}, device_id_type=MESH)
    pl.semaphore_signal(barrier, inc=1, device_id={'tp': partner}, device_id_type=MESH)

    depth = wo_hbm.shape[0]
    o_parts = [(wg, wu)[c // 2].at[o_slot, pl.ds(c % 2 * depth, depth)] for c in range(outs)]
    o_copies = [pltpu.make_async_copy(wo_hbm.at[:, pl.ds(c * OUT_COLS, OUT_COLS)], part, wo_sem.at[c]) for c, part in enumerate(o_parts)]

    chunks = full + (tail > 0)

    def ff_copies(i):
        slot, width = i % FF_SLOTS, min(FF_COLS, inner - i * FF_COLS)
        cols = pl.ds(i * FF_COLS, width)
        return (
            pltpu.make_async_copy(wg_hbm.at[:, cols], wg.at[slot, :, pl.ds(0, width)], g_sem.at[slot]),
            pltpu.make_async_copy(wu_hbm.at[:, cols], wu.at[slot, :, pl.ds(0, width)], u_sem.at[slot]),
        )

    def down_copy(c):
        return pltpu.make_async_copy(wd_hbm.at[:, pl.ds(c * OUT_COLS, OUT_COLS)], wd.at[c], wd_sem.at[c])

    spans = [(k, min(wg.shape[1], inner - k)) for k in range(0, inner, wg.shape[1])]

    def last_down(j):
        first, size = spans[j]
        cols = pl.ds((outs - 1) * OUT_COLS, OUT_COLS)
        return [pltpu.make_async_copy(wd_hbm.at[pl.ds(first, size), cols], wg.at[LAST_SLOT + j, pl.ds(0, size)], last_sem.at[j])]

    def start(copies):
        for copy in copies:
            copy.start()

    def wait(copies):
        for copy in copies:
            copy.wait()

    normed_ref[rows:] = jnp.zeros((PAD_ROWS - rows, normed_ref.shape[1]), BF16)
    act[rows:] = jnp.zeros((PAD_ROWS - rows, act.shape[1]), BF16)
    for copy in small[:3]:
        copy.wait()
    for c in range(SEQ_CHUNKS):
        cache_copy(k_hbm, kbuf, k_sem, c).start()
    for c in range(SEQ_CHUNKS):
        cache_copy(v_hbm, vbuf, v_sem, c).start()

    normed_ref[0:rows] = rms_norm(hidden_ref[...].astype(F32), gain_ref[...].astype(F32)[None, :])
    wait(kv_copies)
    new_rows[...] = dot(normed_ref[...], wkv[...])[:rows].astype(BF16).astype(F32)
    wait(q_copies)
    per_half = FF_COLS // head_dim
    for i, half in enumerate(halves):
        part = dot(normed_ref[...], half[...])[:rows].astype(BF16).astype(F32)
        for h in range(per_half):
            query[:, i * per_half + h, :] = part[:, h * head_dim:(h + 1) * head_dim]
    for i in range(q_slot + 1):
        start(ff_copies(i))

    group = 128 // repeat
    for c in range(rows // group):
        part = slice(c * group, (c + 1) * group)
        hit = jnp.sum(query[part] * new_rows[part, :head_dim][:, None, :], axis=-1, keepdims=True) * scale
        new_scores[part] = jnp.broadcast_to(hit, (group, repeat, block_len))

    lanes = lax.broadcasted_iota(jnp.int32, (repeat, block_len), 1)

    def score_chunk(c):
        for b in range(c * per, (c + 1) * per):
            slot = lens_ref[b] - base
            raw = lax.dot_general(query[b].astype(BF16), kbuf[b], (((1,), (1,)), ((), ())), preferred_element_type=F32)
            fresh = jnp.where(lanes == slot, new_scores[b], -jnp.inf)
            scores[b] = jnp.where(lanes < slot, raw * scale, fresh)

    wait([cache_copy(k_hbm, kbuf, k_sem, c) for c in range(SEQ_CHUNKS)])
    wait([cache_copy(v_hbm, vbuf, v_sem, c) for c in range(SEQ_CHUNKS)])
    for c in range(SEQ_CHUNKS):
        score_chunk(c)

    pairs = lax.broadcasted_iota(jnp.int32, (128, block_len), 1)
    half_pairs = group // 2 * repeat
    low = lax.broadcasted_iota(jnp.int32, (1, 128), 1) < half_pairs
    for c in range(rows // group):
        part = slice(c * group, (c + 1) * group)
        s = scores[part].reshape(128, block_len)
        top = jnp.max(s, axis=-1, keepdims=True)
        p = jnp.where(s > -jnp.inf, jnp.exp(s - top), 0.0)
        total = jnp.sum(p, axis=-1, keepdims=True)
        probs[part] = p.reshape(group, repeat, block_len)
        turned = jnp.where(pairs == 0, top, jnp.where(pairs == 1, total, 0.0)).T
        m_row, l_row = turned[0:1], turned[1:2]
        stats_ref[2 * c] = jnp.where(low, m_row, pltpu.roll(l_row, half_pairs, 1))
        stats_ref[2 * c + 1] = jnp.where(low, pltpu.roll(m_row, half_pairs, 1), l_row)

    def mix_chunk(c):
        for b in range(c * per, (c + 1) * per):
            here = lanes == lens_ref[b] - base
            p = probs[b].astype(BF16).astype(F32)
            fresh = jnp.sum(jnp.where(here, p, 0.0), axis=-1, keepdims=True)
            mix_ref[b] = dot(jnp.where(here, 0.0, p).astype(BF16), vbuf[b]) + fresh * new_rows[b:b + 1, head_dim:]

    for c in range(SEQ_CHUNKS):
        mix_chunk(c)

    pl.semaphore_wait(barrier, n)
    for peer in peers:
        pltpu.make_async_remote_copy(mix_ref.at[peer], got_mix.at[me], mix_send, mix_recv, device_id={'sp': peer}, device_id_type=MESH).start()
        pltpu.make_async_remote_copy(stats_ref.at[peer // per_row], got_stats.at[me], st_send, st_recv, device_id={'sp': peer}, device_id_type=MESH).start()
    got_mix[me] = mix_ref[me]
    got_stats[me] = stats_ref[me // per_row]
    start(o_copies)
    start([down_copy(c) for c in range(outs - 1)])

    tile = lax.broadcasted_iota(jnp.int32, (block_len, head_dim), 0)

    def insert(b, carry):
        here = tile == lens_ref[b] - base
        new = new_rows[pl.ds(b, 1), :].astype(BF16)
        kbuf[b] = jnp.where(here, jnp.broadcast_to(new[:, :head_dim], here.shape), kbuf[b])
        vbuf[b] = jnp.where(here, jnp.broadcast_to(new[:, head_dim:], here.shape), vbuf[b])
        return carry

    lax.fori_loop(0, rows, insert, 0)

    def bulk(ref, send, recv):
        span = ref.at[pl.ds(0, n - 1)]
        return pltpu.make_async_remote_copy(span, span, send, recv, device_id={'tp': partner}, device_id_type=MESH)

    bulk(got_stats, st_send, st_recv).wait_recv()
    flipped[...] = got_stats[:, 0, :].T
    first = pl.multiple_of(lax.rem(me, per_row) * repeat, repeat)
    tops = flipped[pl.ds(first, repeat), :]
    totals = flipped[pl.ds(pl.multiple_of(per_row * repeat + first, repeat), repeat), :]
    factor = jnp.exp(tops - jnp.max(tops, axis=-1, keepdims=True))
    total = jnp.sum(factor * totals, axis=-1, keepdims=True)
    bulk(got_mix, mix_send, mix_recv).wait_recv()
    ways = 4
    sums = [factor[:, s:s + 1] * got_mix[s] for s in range(ways)]
    for s in range(ways, n):
        sums[s % ways] = sums[s % ways] + factor[:, s:s + 1] * got_mix[s]
    mixed = (sums[0] + sums[1]) + (sums[2] + sums[3])
    row = (mixed / total).astype(BF16).astype(F32)
    own[...] = row
    gathered[me] = row
    for peer in peers:
        pltpu.make_async_remote_copy(own, gathered.at[me], own_send, own_recv, device_id={'sp': peer}, device_id_type=MESH).start()
    small[3].wait()
    wait(o_copies)
    bulk(gathered, own_send, own_recv).wait_recv()
    attended = jnp.concatenate([gathered[:, h, :] for h in range(repeat)], axis=-1).astype(BF16)
    attended = jnp.concatenate([attended, jnp.zeros((PAD_ROWS - rows, attended.shape[1]), BF16)], axis=0)

    def exchange(mine, theirs, send, recv, c):
        return pltpu.make_async_remote_copy(mine.at[c], theirs.at[c], send.at[c], recv.at[c], device_id={'tp': partner}, device_id_type=MESH)

    for c in range(outs):
        sent[c] = dot(attended, o_parts[c][...])[:rows]
        exchange(sent, other, o_send, o_recv, c).start()
    for i in range(o_slot, FF_SLOTS):
        start(ff_copies(i))
    for c in range(outs):
        exchange(sent, other, o_send, o_recv, c).wait_recv()
        cols = slice(c * OUT_COLS, (c + 1) * OUT_COLS)
        mid_ref[:, cols] = (hidden_ref[:, cols].astype(F32) + (sent[c] + other[c])).astype(BF16)
    normed_ref[0:rows] = rms_norm(mid_ref[...].astype(F32), gain2_ref[...].astype(F32)[None, :])

    def inner_step(i):
        slot, width = i % FF_SLOTS, min(FF_COLS, inner - i * FF_COLS)
        gate = dot(normed_ref[...], wg[slot, :, :width])[:rows]
        up = dot(normed_ref[...], wu[slot, :, :width])[:rows]
        act[0:rows, i * FF_COLS:i * FF_COLS + width] = (jax.nn.silu(gate) * up).astype(BF16)
        if i + FF_SLOTS < chunks:
            start(ff_copies(i + FF_SLOTS))
        if 0 <= i - LAST_SLOT < len(spans):
            start(last_down(i - LAST_SLOT))

    for lo, hi in FF_GROUPS:
        for i in range(lo, min(hi, chunks)):
            wait(ff_copies(i))
        for i in range(lo, min(hi, chunks)):
            inner_step(i)

    wait([down_copy(c) for c in range(outs - 1)])
    for c in range(outs - 1):
        sent2[c] = dot(act[...], wd[c])[:rows]
        exchange(sent2, other2, d_send, d_recv, c).start()
    for j in range(len(spans)):
        wait(last_down(j))
    pieces = [dot(act[:, first:first + size], wg[LAST_SLOT + j, :size])[:rows] for j, (first, size) in enumerate(spans)]
    sent2[outs - 1] = sum(pieces[1:], pieces[0])
    exchange(sent2, other2, d_send, d_recv, outs - 1).start()
    for c in range(outs):
        exchange(sent2, other2, d_send, d_recv, c).wait_recv()
        cols = slice(c * OUT_COLS, (c + 1) * OUT_COLS)
        out_ref[:, cols] = (mid_ref[:, cols].astype(F32) + (sent2[c] + other2[c])).astype(BF16)

    bulk(got_mix, mix_send, mix_recv).wait_send()
    bulk(got_stats, st_send, st_recv).wait_send()
    bulk(gathered, own_send, own_recv).wait_send()
    for c in range(outs):
        exchange(sent, other, o_send, o_recv, c).wait_send()
        exchange(sent2, other2, d_send, d_recv, c).wait_send()


def layer(seq_lens, hidden, gain, gain2, w_q, w_k, w_v, k_cache, v_cache, w_o, w_gate, w_up, w_down):
    rows, block_len, head_dim = k_cache.shape
    repeat = w_q.shape[1] // head_dim
    width = w_o.shape[1]
    inner = w_gate.shape[1]
    outs = width // OUT_COLS
    assert w_q.shape[1] == 2 * FF_COLS
    raw = pl.BlockSpec(memory_space=pltpu.HBM)
    whole = pl.BlockSpec(memory_space=pltpu.VMEM)
    dma = pltpu.SemaphoreType.DMA
    heads = (rows, repeat, head_dim)
    return pl.pallas_call(
        layer_kernel,
        name='layer',
        out_shape=(pltpu.VMEM(hidden.shape, BF16), pltpu.VMEM(k_cache.shape, BF16), pltpu.VMEM(v_cache.shape, BF16)),
        in_specs=[raw] * 13,
        out_specs=(whole, whole, whole),
        scratch_shapes=[
            pltpu.SMEM(seq_lens.shape, jnp.int32),
            pltpu.VMEM(hidden.shape, BF16),
            pltpu.VMEM(gain.shape, BF16),
            pltpu.VMEM(gain2.shape, BF16),
            pltpu.VMEM(heads, F32),
            pltpu.VMEM((rows, 2 * head_dim), F32),
            pltpu.VMEM((rows, repeat, block_len), F32),
            pltpu.VMEM((rows, repeat, block_len), F32),
            pltpu.VMEM((rows, repeat, block_len), F32),
            pltpu.VMEM(heads, F32),
            pltpu.VMEM((2 * rows * repeat // 128, 1, 128), F32),
            pltpu.VMEM(heads, F32),
            pltpu.VMEM((rows, 1, 128), F32),
            pltpu.VMEM((128, rows), F32),
            pltpu.VMEM((repeat, head_dim), F32),
            pltpu.VMEM(heads, F32),
            pltpu.VMEM((FF_SLOTS, width, FF_COLS), BF16),
            pltpu.VMEM((FF_SLOTS, width, FF_COLS), BF16),
            pltpu.VMEM((outs - 1, inner, OUT_COLS), BF16),
            pltpu.VMEM((outs, rows, OUT_COLS), F32),
            pltpu.VMEM((outs, rows, OUT_COLS), F32),
            pltpu.VMEM((rows, width), BF16),
            pltpu.VMEM((PAD_ROWS, width), BF16),
            pltpu.VMEM((PAD_ROWS, inner), BF16),
            pltpu.VMEM((outs, rows, OUT_COLS), F32),
            pltpu.VMEM((outs, rows, OUT_COLS), F32),
            dma, dma, dma, dma, dma, dma,
            dma((outs,)), dma((outs,)), dma((outs,)), dma((outs,)),
            dma((4,)), dma((2,)), dma((2,)), dma((SEQ_CHUNKS,)), dma((SEQ_CHUNKS,)),
            dma((outs,)), dma((FF_SLOTS,)), dma((FF_SLOTS,)), dma((outs - 1,)), dma((-(-inner // width),)),
        ],
        compiler_params=pltpu.CompilerParams(collective_id=0, has_side_effects=True, vmem_limit_bytes=59 << 20),
    )(*stay(seq_lens, hidden, gain, gain2, w_q, w_k, w_v, k_cache, v_cache, w_o, w_gate, w_up, w_down))


def write_kernel(*refs):
    count = len(refs) // 2
    sems = refs[-1]
    copies = [pltpu.make_async_copy(refs[i], refs[count + i], sems.at[i]) for i in range(count)]
    for copy in copies:
        copy.start()
    for copy in copies:
        copy.wait()


def write(*arrays):
    return pl.pallas_call(
        write_kernel,
        name='write',
        out_shape=tuple(pltpu.HBM(x.shape, x.dtype) for x in arrays),
        in_specs=[pl.BlockSpec(memory_space=pltpu.VMEM)] * len(arrays),
        out_specs=tuple(pl.BlockSpec(memory_space=pltpu.HBM) for _ in arrays),
        scratch_shapes=[pltpu.SemaphoreType.DMA((len(arrays),))],
        compiler_params=pltpu.CompilerParams(vmem_limit_bytes=4 << 20),
    )(*stay(*arrays, space=pltpu.VMEM))


def solution(mesh):
    cache_spec = P('dp', 'tp', 'sp', None)
    row_spec = P('dp', None)
    col_spec = P(None, 'tp')
    inner_spec = P('tp', None)
    gain_spec = P(None)

    def local_step(hidden, seq_lens, k_cache, v_cache, attn_norm, w_q, w_k, w_v, w_o, mlp_norm, w_gate, w_up, w_down):
        shape = k_cache.shape
        flat = (shape[0] * shape[1], shape[2], shape[3])
        parts = layer(seq_lens, hidden, attn_norm, mlp_norm, w_q, w_k, w_v, k_cache.reshape(flat), v_cache.reshape(flat), w_o, w_gate, w_up, w_down)
        hidden_out, k_out, v_out = write(*parts)
        return hidden_out, k_out.reshape(shape), v_out.reshape(shape)

    return jax.shard_map(local_step, mesh=mesh, in_specs=(row_spec, P('dp'), cache_spec, cache_spec, gain_spec, col_spec, col_spec, col_spec, inner_spec, gain_spec, col_spec, col_spec, inner_spec), out_specs=(row_spec, cache_spec, cache_spec), check_vma=False)
```

```python
import itertools

import jax
import jax.numpy as jnp
from jax import lax
from jax.experimental import pallas as pl
from jax.experimental.pallas import tpu as pltpu
from jax.sharding import PartitionSpec as P

NORM_EPS = 1e-6
MESH = pl.DeviceIdType.MESH
F32 = jnp.float32
BF16 = jnp.bfloat16
SEQ_CHUNKS = 4
PAD_ROWS = 128
FF_COLS = 512
FF_SLOTS = 8
OUT_COLS = 512
FF_GROUPS = ((0, 7), (7, 9), (9, 11))
LAST_SLOT = 3


def rms_norm(wide, gain):
    scaled = wide * lax.rsqrt(jnp.mean(wide * wide, axis=-1, keepdims=True) + NORM_EPS)
    return (scaled * gain).astype(BF16)


def dot(a, b):
    return jnp.dot(a, b, preferred_element_type=F32)


def stay(*arrays, space=pltpu.HBM):
    return [pltpu.with_memory_space_constraint(x, space) for x in arrays]


def layer_kernel(lens_hbm, hidden_hbm, gain_hbm, gain2_hbm, wq_hbm, wk_hbm, wv_hbm, k_hbm, v_hbm, wo_hbm, wg_hbm, wu_hbm, wd_hbm,
                 out_ref, kbuf, vbuf,
                 lens_ref, hidden_ref, gain_ref, gain2_ref, query, new_rows, new_scores, scores, probs, mix_ref, stats_ref,
                 got_mix, got_stats, flipped, own, gathered, wg, wu, wd, sent, other, mid_ref, normed_ref, act, sent2, other2,
                 mix_send, mix_recv, st_send, st_recv, own_send, own_recv, o_send, o_recv, d_send, d_recv,
                 small_sem, w_sem, q_sem, k_sem, v_sem, wo_sem, g_sem, u_sem, wd_sem, last_sem):
    rows, block_len, head_dim = kbuf.shape
    repeat = mix_ref.shape[1]
    n = rows
    me = lax.axis_index('sp')
    partner = 1 - lax.axis_index('tp')
    base = me * block_len
    scale = head_dim ** -0.5
    per = rows // SEQ_CHUNKS
    inner = wg_hbm.shape[1]
    full = inner // FF_COLS
    tail = inner - full * FF_COLS
    outs = wo_hbm.shape[1] // OUT_COLS
    per_row = 128 // (2 * repeat)

    small = [pltpu.make_async_copy(src, dst, small_sem.at[i]) for i, (src, dst) in enumerate(
        ((hidden_hbm, hidden_ref), (gain_hbm, gain_ref), (lens_hbm, lens_ref), (gain2_hbm, gain2_ref)))]
    for copy in small:
        copy.start()

    wkv = wd.at[outs - 2, pl.ds(0, wk_hbm.shape[0]), pl.ds(0, 2 * head_dim)]
    kv_copies = [pltpu.make_async_copy(src, wd.at[outs - 2, pl.ds(0, wk_hbm.shape[0])].at[:, pl.ds(i * head_dim, head_dim)], w_sem.at[i]) for i, src in enumerate((wk_hbm, wv_hbm))]
    for copy in kv_copies:
        copy.start()
    q_slot, o_slot = FF_SLOTS - 2, FF_SLOTS - 1
    halves = (wg.at[q_slot], wu.at[q_slot])
    q_copies = [pltpu.make_async_copy(wq_hbm.at[:, pl.ds(i * FF_COLS, FF_COLS)], half, q_sem.at[i]) for i, half in enumerate(halves)]
    for copy in q_copies:
        copy.start()

    def cache_copy(hbm, buf, sems, c):
        part = pl.ds(c * per, per)
        return pltpu.make_async_copy(hbm.at[part], buf.at[part], sems.at[c])

    barrier = pltpu.get_barrier_semaphore()
    side = round(n ** (1 / 3))
    xs = [lax.rem(lax.rem(me, side) + d, side) for d in range(side)]
    ys = [lax.rem(lax.rem(me // side, side) + d, side) * side for d in range(side)]
    zs = [lax.rem(me // (side * side) + d, side) * (side * side) for d in range(side)]
    hops = lambda o: sum(min(d, side - d) for d in o)
    offsets = sorted(itertools.product(range(side), repeat=3), key=hops, reverse=True)[:-1]
    peers = [xs[a] + ys[b] + zs[c] for a, b, c in offsets]
    for peer in peers:
        pl.semaphore_signal(barrier, inc=1, device_id={'sp': peer}, device_id_type=MESH)
    pl.semaphore_signal(barrier, inc=1, device_id={'tp': partner}, device_id_type=MESH)

    depth = wo_hbm.shape[0]
    o_parts = [(wg, wu)[c // 2].at[o_slot, pl.ds(c % 2 * depth, depth)] for c in range(outs)]
    o_copies = [pltpu.make_async_copy(wo_hbm.at[:, pl.ds(c * OUT_COLS, OUT_COLS)], part, wo_sem.at[c]) for c, part in enumerate(o_parts)]

    chunks = full + (tail > 0)

    def ff_copies(i):
        slot, width = i % FF_SLOTS, min(FF_COLS, inner - i * FF_COLS)
        cols = pl.ds(i * FF_COLS, width)
        return (
            pltpu.make_async_copy(wg_hbm.at[:, cols], wg.at[slot, :, pl.ds(0, width)], g_sem.at[slot]),
            pltpu.make_async_copy(wu_hbm.at[:, cols], wu.at[slot, :, pl.ds(0, width)], u_sem.at[slot]),
        )

    def down_copy(c):
        return pltpu.make_async_copy(wd_hbm.at[:, pl.ds(c * OUT_COLS, OUT_COLS)], wd.at[c], wd_sem.at[c])

    spans = [(k, min(wg.shape[1], inner - k)) for k in range(0, inner, wg.shape[1])]

    def last_down(j):
        first, size = spans[j]
        cols = pl.ds((outs - 1) * OUT_COLS, OUT_COLS)
        return [pltpu.make_async_copy(wd_hbm.at[pl.ds(first, size), cols], wg.at[LAST_SLOT + j, pl.ds(0, size)], last_sem.at[j])]

    def start(copies):
        for copy in copies:
            copy.start()

    def wait(copies):
        for copy in copies:
            copy.wait()

    normed_ref[rows:] = jnp.zeros((PAD_ROWS - rows, normed_ref.shape[1]), BF16)
    act[rows:] = jnp.zeros((PAD_ROWS - rows, act.shape[1]), BF16)
    for copy in small[:3]:
        copy.wait()
    for c in range(SEQ_CHUNKS):
        cache_copy(k_hbm, kbuf, k_sem, c).start()
    for c in range(SEQ_CHUNKS):
        cache_copy(v_hbm, vbuf, v_sem, c).start()

    normed_ref[0:rows] = rms_norm(hidden_ref[...].astype(F32), gain_ref[...].astype(F32)[None, :])
    wait(kv_copies)
    new_rows[...] = dot(normed_ref[...], wkv[...])[:rows].astype(BF16).astype(F32)
    wait(q_copies)
    per_half = FF_COLS // head_dim
    for i, half in enumerate(halves):
        part = dot(normed_ref[...], half[...])[:rows].astype(BF16).astype(F32)
        for h in range(per_half):
            query[:, i * per_half + h, :] = part[:, h * head_dim:(h + 1) * head_dim]
    for i in range(q_slot + 1):
        start(ff_copies(i))

    group = 128 // repeat
    for c in range(rows // group):
        part = slice(c * group, (c + 1) * group)
        hit = jnp.sum(query[part] * new_rows[part, :head_dim][:, None, :], axis=-1, keepdims=True) * scale
        new_scores[part] = jnp.broadcast_to(hit, (group, repeat, block_len))

    lanes = lax.broadcasted_iota(jnp.int32, (repeat, block_len), 1)

    def score_chunk(c):
        for b in range(c * per, (c + 1) * per):
            slot = lens_ref[b] - base
            raw = lax.dot_general(query[b].astype(BF16), kbuf[b], (((1,), (1,)), ((), ())), preferred_element_type=F32)
            fresh = jnp.where(lanes == slot, new_scores[b], -jnp.inf)
            scores[b] = jnp.where(lanes < slot, raw * scale, fresh)

    wait([cache_copy(k_hbm, kbuf, k_sem, c) for c in range(SEQ_CHUNKS)])
    wait([cache_copy(v_hbm, vbuf, v_sem, c) for c in range(SEQ_CHUNKS)])
    for c in range(SEQ_CHUNKS):
        score_chunk(c)

    pairs = lax.broadcasted_iota(jnp.int32, (128, block_len), 1)
    half_pairs = group // 2 * repeat
    low = lax.broadcasted_iota(jnp.int32, (1, 128), 1) < half_pairs
    for c in range(rows // group):
        part = slice(c * group, (c + 1) * group)
        s = scores[part].reshape(128, block_len)
        top = jnp.max(s, axis=-1, keepdims=True)
        p = jnp.where(s > -jnp.inf, jnp.exp(s - top), 0.0)
        total = jnp.sum(p, axis=-1, keepdims=True)
        probs[part] = p.reshape(group, repeat, block_len)
        turned = jnp.where(pairs == 0, top, jnp.where(pairs == 1, total, 0.0)).T
        m_row, l_row = turned[0:1], turned[1:2]
        stats_ref[2 * c] = jnp.where(low, m_row, pltpu.roll(l_row, half_pairs, 1))
        stats_ref[2 * c + 1] = jnp.where(low, pltpu.roll(m_row, half_pairs, 1), l_row)

    def mix_chunk(c):
        for b in range(c * per, (c + 1) * per):
            here = lanes == lens_ref[b] - base
            p = probs[b].astype(BF16).astype(F32)
            fresh = jnp.sum(jnp.where(here, p, 0.0), axis=-1, keepdims=True)
            mix_ref[b] = dot(jnp.where(here, 0.0, p).astype(BF16), vbuf[b]) + fresh * new_rows[b:b + 1, head_dim:]

    for c in range(SEQ_CHUNKS):
        mix_chunk(c)

    pl.semaphore_wait(barrier, n)
    for peer in peers:
        pltpu.make_async_remote_copy(mix_ref.at[peer], got_mix.at[me], mix_send, mix_recv, device_id={'sp': peer}, device_id_type=MESH).start()
        pltpu.make_async_remote_copy(stats_ref.at[peer // per_row], got_stats.at[me], st_send, st_recv, device_id={'sp': peer}, device_id_type=MESH).start()
    got_mix[me] = mix_ref[me]
    got_stats[me] = stats_ref[me // per_row]
    start(o_copies)
    start([down_copy(c) for c in range(outs - 1)])

    tile = lax.broadcasted_iota(jnp.int32, (block_len, head_dim), 0)

    def insert(b, carry):
        here = tile == lens_ref[b] - base
        new = new_rows[pl.ds(b, 1), :].astype(BF16)
        kbuf[b] = jnp.where(here, jnp.broadcast_to(new[:, :head_dim], here.shape), kbuf[b])
        vbuf[b] = jnp.where(here, jnp.broadcast_to(new[:, head_dim:], here.shape), vbuf[b])
        return carry

    lax.fori_loop(0, rows, insert, 0)

    def bulk(ref, send, recv):
        span = ref.at[pl.ds(0, n - 1)]
        return pltpu.make_async_remote_copy(span, span, send, recv, device_id={'tp': partner}, device_id_type=MESH)

    bulk(got_stats, st_send, st_recv).wait_recv()
    spread = new_scores
    flipped[...] = got_stats[:, 0, :].T
    first = pl.multiple_of(lax.rem(me, per_row) * repeat, repeat)
    tops = flipped[pl.ds(first, repeat), :]
    totals = flipped[pl.ds(pl.multiple_of(per_row * repeat + first, repeat), repeat), :]
    factor = jnp.exp(tops - jnp.max(tops, axis=-1, keepdims=True))
    total = jnp.sum(factor * totals, axis=-1, keepdims=True)
    for s in range(n):
        spread[s] = jnp.broadcast_to(factor[:, s:s + 1], (repeat, head_dim))
    bulk(got_mix, mix_send, mix_recv).wait_recv()
    ways = 4
    sums = [spread[s] * got_mix[s] for s in range(ways)]
    for s in range(ways, n):
        sums[s % ways] = sums[s % ways] + spread[s] * got_mix[s]
    mixed = (sums[0] + sums[1]) + (sums[2] + sums[3])
    row = (mixed / total).astype(BF16).astype(F32)
    own[...] = row
    gathered[me] = row
    for peer in peers:
        pltpu.make_async_remote_copy(own, gathered.at[me], own_send, own_recv, device_id={'sp': peer}, device_id_type=MESH).start()
    small[3].wait()
    wait(o_copies)
    bulk(gathered, own_send, own_recv).wait_recv()
    attended = jnp.concatenate([gathered[:, h, :] for h in range(repeat)], axis=-1).astype(BF16)
    attended = jnp.concatenate([attended, jnp.zeros((PAD_ROWS - rows, attended.shape[1]), BF16)], axis=0)

    def exchange(mine, theirs, send, recv, c):
        return pltpu.make_async_remote_copy(mine.at[c], theirs.at[c], send.at[c], recv.at[c], device_id={'tp': partner}, device_id_type=MESH)

    for c in range(outs):
        sent[c] = dot(attended, o_parts[c][...])[:rows]
        if c:
            exchange(sent, other, o_send, o_recv, c - 1).start()
    exchange(sent, other, o_send, o_recv, outs - 1).start()
    for i in range(o_slot, FF_SLOTS):
        start(ff_copies(i))
    square = jnp.zeros((rows, 1), F32)
    for c in range(outs):
        exchange(sent, other, o_send, o_recv, c).wait_recv()
        cols = slice(c * OUT_COLS, (c + 1) * OUT_COLS)
        mid = (hidden_ref[:, cols].astype(F32) + (sent[c] + other[c])).astype(BF16)
        mid_ref[:, cols] = mid
        square = square + jnp.sum(jnp.square(mid.astype(F32)), axis=-1, keepdims=True)
    shrink = lax.rsqrt(square / mid_ref.shape[1] + NORM_EPS)
    normed_ref[0:rows] = (mid_ref[...].astype(F32) * shrink * gain2_ref[...].astype(F32)[None, :]).astype(BF16)

    def inner_step(i):
        slot, width = i % FF_SLOTS, min(FF_COLS, inner - i * FF_COLS)
        gate = dot(normed_ref[...], wg[slot, :, :width])[:rows]
        up = dot(normed_ref[...], wu[slot, :, :width])[:rows]
        act[0:rows, i * FF_COLS:i * FF_COLS + width] = (jax.nn.silu(gate) * up).astype(BF16)
        if i + FF_SLOTS < chunks:
            start(ff_copies(i + FF_SLOTS))
        if 0 <= i - LAST_SLOT < len(spans):
            start(last_down(i - LAST_SLOT))

    for lo, hi in FF_GROUPS:
        for i in range(lo, min(hi, chunks)):
            wait(ff_copies(i))
        for i in range(lo, min(hi, chunks)):
            inner_step(i)

    wait([down_copy(c) for c in range(outs - 1)])
    for c in range(outs - 1):
        sent2[c] = dot(act[...], wd[c])[:rows]
        if c:
            exchange(sent2, other2, d_send, d_recv, c - 1).start()
    exchange(sent2, other2, d_send, d_recv, outs - 2).start()
    for j in range(len(spans)):
        wait(last_down(j))
    pieces = [dot(act[:, first:first + size], wg[LAST_SLOT + j, :size])[:rows] for j, (first, size) in enumerate(spans)]
    sent2[outs - 1] = sum(pieces[1:], pieces[0])
    exchange(sent2, other2, d_send, d_recv, outs - 1).start()
    for c in range(outs):
        exchange(sent2, other2, d_send, d_recv, c).wait_recv()
        cols = slice(c * OUT_COLS, (c + 1) * OUT_COLS)
        out_ref[:, cols] = (mid_ref[:, cols].astype(F32) + (sent2[c] + other2[c])).astype(BF16)

    bulk(got_mix, mix_send, mix_recv).wait_send()
    bulk(got_stats, st_send, st_recv).wait_send()
    bulk(gathered, own_send, own_recv).wait_send()
    for c in range(outs):
        exchange(sent, other, o_send, o_recv, c).wait_send()
        exchange(sent2, other2, d_send, d_recv, c).wait_send()


def layer(seq_lens, hidden, gain, gain2, w_q, w_k, w_v, k_cache, v_cache, w_o, w_gate, w_up, w_down):
    rows, block_len, head_dim = k_cache.shape
    repeat = w_q.shape[1] // head_dim
    width = w_o.shape[1]
    inner = w_gate.shape[1]
    outs = width // OUT_COLS
    assert w_q.shape[1] == 2 * FF_COLS
    raw = pl.BlockSpec(memory_space=pltpu.HBM)
    whole = pl.BlockSpec(memory_space=pltpu.VMEM)
    dma = pltpu.SemaphoreType.DMA
    heads = (rows, repeat, head_dim)
    return pl.pallas_call(
        layer_kernel,
        name='layer',
        out_shape=(pltpu.VMEM(hidden.shape, BF16), pltpu.VMEM(k_cache.shape, BF16), pltpu.VMEM(v_cache.shape, BF16)),
        in_specs=[raw] * 13,
        out_specs=(whole, whole, whole),
        scratch_shapes=[
            pltpu.SMEM(seq_lens.shape, jnp.int32),
            pltpu.VMEM(hidden.shape, BF16),
            pltpu.VMEM(gain.shape, BF16),
            pltpu.VMEM(gain2.shape, BF16),
            pltpu.VMEM(heads, F32),
            pltpu.VMEM((rows, 2 * head_dim), F32),
            pltpu.VMEM((rows, repeat, block_len), F32),
            pltpu.VMEM((rows, repeat, block_len), F32),
            pltpu.VMEM((rows, repeat, block_len), F32),
            pltpu.VMEM(heads, F32),
            pltpu.VMEM((2 * rows * repeat // 128, 1, 128), F32),
            pltpu.VMEM(heads, F32),
            pltpu.VMEM((rows, 1, 128), F32),
            pltpu.VMEM((128, rows), F32),
            pltpu.VMEM((repeat, head_dim), F32),
            pltpu.VMEM(heads, F32),
            pltpu.VMEM((FF_SLOTS, width, FF_COLS), BF16),
            pltpu.VMEM((FF_SLOTS, width, FF_COLS), BF16),
            pltpu.VMEM((outs - 1, inner, OUT_COLS), BF16),
            pltpu.VMEM((outs, rows, OUT_COLS), F32),
            pltpu.VMEM((outs, rows, OUT_COLS), F32),
            pltpu.VMEM((rows, width), BF16),
            pltpu.VMEM((PAD_ROWS, width), BF16),
            pltpu.VMEM((PAD_ROWS, inner), BF16),
            pltpu.VMEM((outs, rows, OUT_COLS), F32),
            pltpu.VMEM((outs, rows, OUT_COLS), F32),
            dma, dma, dma, dma, dma, dma,
            dma((outs,)), dma((outs,)), dma((outs,)), dma((outs,)),
            dma((4,)), dma((2,)), dma((2,)), dma((SEQ_CHUNKS,)), dma((SEQ_CHUNKS,)),
            dma((outs,)), dma((FF_SLOTS,)), dma((FF_SLOTS,)), dma((outs - 1,)), dma((-(-inner // width),)),
        ],
        compiler_params=pltpu.CompilerParams(collective_id=0, has_side_effects=True, vmem_limit_bytes=59 << 20),
    )(*stay(seq_lens, hidden, gain, gain2, w_q, w_k, w_v, k_cache, v_cache, w_o, w_gate, w_up, w_down))


def write_kernel(*refs):
    count = len(refs) // 2
    sems = refs[-1]
    copies = [pltpu.make_async_copy(refs[i], refs[count + i], sems.at[i]) for i in range(count)]
    for copy in copies:
        copy.start()
    for copy in copies:
        copy.wait()


def write(*arrays):
    return pl.pallas_call(
        write_kernel,
        name='write',
        out_shape=tuple(pltpu.HBM(x.shape, x.dtype) for x in arrays),
        in_specs=[pl.BlockSpec(memory_space=pltpu.VMEM)] * len(arrays),
        out_specs=tuple(pl.BlockSpec(memory_space=pltpu.HBM) for _ in arrays),
        scratch_shapes=[pltpu.SemaphoreType.DMA((len(arrays),))],
        compiler_params=pltpu.CompilerParams(vmem_limit_bytes=4 << 20),
    )(*stay(*arrays, space=pltpu.VMEM))


def solution(mesh):
    cache_spec = P('dp', 'tp', 'sp', None)
    row_spec = P('dp', None)
    col_spec = P(None, 'tp')
    inner_spec = P('tp', None)
    gain_spec = P(None)

    def local_step(hidden, seq_lens, k_cache, v_cache, attn_norm, w_q, w_k, w_v, w_o, mlp_norm, w_gate, w_up, w_down):
        shape = k_cache.shape
        flat = (shape[0] * shape[1], shape[2], shape[3])
        parts = layer(seq_lens, hidden, attn_norm, mlp_norm, w_q, w_k, w_v, k_cache.reshape(flat), v_cache.reshape(flat), w_o, w_gate, w_up, w_down)
        hidden_out, k_out, v_out = write(*parts)
        return hidden_out, k_out.reshape(shape), v_out.reshape(shape)

    return jax.shard_map(local_step, mesh=mesh, in_specs=(row_spec, P('dp'), cache_spec, cache_spec, gain_spec, col_spec, col_spec, col_spec, inner_spec, gain_spec, col_spec, col_spec, inner_spec), out_specs=(row_spec, cache_spec, cache_spec), check_vma=False)
```
